128 devices in a mesh: section: 2 (over x_hi), dp: 16 (over z, y), mp: 4 (over x_lo, core).
Axes of the slice: x: 4 (x_hi: 2, x_lo: 2; x = x_hi * 2 + x_lo), y: 4, z: 4, core: 2. Of those that a mesh axis runs over, the one named last changes fastest.
Arguments:
- text_feats: bfloat16 [16384, 512], P('dp'), may hold values from -48 to 48
- image_feats: bfloat16 [16384, 512], P(('dp', 'mp')), may hold values from -48 to 48
- logit_scale: float32 [1], replicated, may hold values from 10 to 320
- layer_inputs: bfloat16 [2, 16384, 512], P('section', 'dp'), may hold values from -6 to 6
- w_in: bfloat16 [2, 512, 2048], P('section', None, 'mp'), may hold values from -0.25 to 0.25
- w_out: bfloat16 [2, 2048, 512], P('section', 'mp'), may hold values from -0.125 to 0.125
Outputs:
- image_grad: bfloat16 [16384, 512], P(('dp', 'mp'))
- input_grad: bfloat16 [16384, 512], P('dp', 'section')
- w_in_grad: float32 [2, 512, 2048], P('section', 'dp', 'mp')
- w_out_grad_t: float32 [2, 512, 2048], P('section', 'dp', 'mp')
The draws below stay inside these ranges and needn't reach their ends.
All inputs are finite; a program needn't handle non-finite values.
Results may differ from the reference program's by a relative error of at most 0.017.
Values may be sent and summed in bfloat16 or wider, within the bound.
A program may use at most 128 MiB of HBM per device.

```python
import jax
import jax.numpy as jnp
from jax import lax

D = 512
FF = 2048
PAIRS_DEV = 1024
PAIRS = 16384
LAYERS = 2


def joint_feats(key):
    folded = jax.random.fold_in(key, 11)
    key_shared, key_text, key_image, key_scale = jax.random.split(folded, 4)
    shared = jnp.clip(jax.random.normal(key_shared, (PAIRS, D), jnp.float32), -4.0, 4.0)
    text_noise = jnp.clip(jax.random.normal(key_text, (PAIRS, D), jnp.float32), -4.0, 4.0)
    image_noise = jnp.clip(jax.random.normal(key_image, (PAIRS, D), jnp.float32), -4.0, 4.0)
    text_rows = shared + text_noise
    image_rows = shared + image_noise
    return (text_rows, image_rows)


def draw_text_feats(key, part):
    text_rows, image_rows = joint_feats(key)
    return text_rows.astype(jnp.bfloat16)


def draw_image_feats(key, part):
    text_rows, image_rows = joint_feats(key)
    return image_rows.astype(jnp.bfloat16)


def draw_logit_scale(key, part):
    folded = jax.random.fold_in(key, 23)
    return jax.random.uniform(folded, (1,), jnp.float32, 10.0, 30.0)


def block_levels(rng, dims, cuts, smallest, top_value):
    factor_of, own = 1.0, jax.random.fold_in(rng, 6)
    for dim, parts in cuts:
        steps = jnp.exp(jax.random.uniform(jax.random.fold_in(own, dim), (parts,), jnp.float32, smallest / len(cuts), top_value / len(cuts)))
        factor_of = factor_of * jnp.repeat(steps, dims[dim] // parts).reshape([-1 if axis == dim else 1 for axis in range(len(dims))])
    return factor_of


def gaussian(key, extent, deviation, limit, cuts=(), kind=jnp.bfloat16):
    entries = jax.random.normal(key, extent, jnp.float32) * deviation
    if len(cuts) > 0:
        entries = block_levels(key, extent, cuts, -0.22, 0.18) * entries
    return jnp.clip(entries, min=-limit, max=limit).astype(kind)


def setup_inputs(seed: int = 0) -> dict:
    splits = jax.random.split(jax.random.key(seed), 7)
    text_feats = draw_text_feats(jax.random.fold_in(splits[6], 71), 0)
    image_feats = draw_image_feats(jax.random.fold_in(splits[6], 71), 0)
    logit_scale = draw_logit_scale(jax.random.fold_in(splits[6], 71), 0)
    layer_inputs = gaussian(splits[3], (LAYERS, PAIRS, D), 1.0, 6.0, ((0, 2), (1, 16)))
    w_in = gaussian(splits[4], (LAYERS, D, FF), D ** -0.5, 0.25, ((0, 2), (2, 4)))
    w_out = gaussian(splits[5], (LAYERS, FF, D), FF ** -0.5, 0.125, ((0, 2), (1, 4)))
    return {"text_feats": text_feats, "image_feats": image_feats, "logit_scale": logit_scale, "layer_inputs": layer_inputs, "w_in": w_in, "w_out": w_out}


def unit_rows(values):
    wide = values.astype(jnp.float32)
    length = jnp.sqrt(lax.optimization_barrier(jnp.sum(wide * wide, axis=1, keepdims=True)) + 1.0)
    return (wide / length, length)

def unit_backward(unit, length, grad_unit):
    return (grad_unit - unit * lax.optimization_barrier(jnp.sum(unit * grad_unit, axis=1, keepdims=True))) / length

def quick_gelu(values):
    return values * jax.nn.sigmoid(1.702 * values)

def quick_slope(values):
    sigm = jax.nn.sigmoid(1.702 * values)
    return sigm + 1.702 * values * sigm * (1.0 - sigm)

def reference(text_feats, image_feats, logit_scale, layer_inputs, w_in, w_out):
    logit_mult = logit_scale[0]
    text_unit, text_length = unit_rows(text_feats)
    image_unit, image_length = unit_rows(image_feats)
    text_low = text_unit.astype(jnp.bfloat16)
    image_low = image_unit.astype(jnp.bfloat16)
    block_count = PAIRS // PAIRS_DEV
    text_blocks = text_low.reshape(block_count, PAIRS_DEV, D)
    block_ids = jnp.arange(block_count, dtype=jnp.int32)
    column_ids = jnp.arange(PAIRS, dtype=jnp.int32)

    def stats_step(state_pair, text_block):
        column_peak, column_total = state_pair
        scores = logit_mult * jnp.dot(text_block, image_low.T, preferred_element_type=jnp.float32)
        row_peak = lax.optimization_barrier(jnp.max(scores, axis=1))
        row_total = lax.optimization_barrier(jnp.sum(jnp.exp(scores - row_peak[:, None]), axis=1))
        new_peak = jnp.maximum(column_peak, lax.optimization_barrier(jnp.max(scores, axis=0)))
        column_total = column_total * jnp.exp(column_peak - new_peak) + lax.optimization_barrier(jnp.sum(jnp.exp(scores - new_peak[None, :]), axis=0))
        return ((new_peak, column_total), (row_peak, row_total))
    start_pair = (jnp.full((PAIRS,), -1e+30, jnp.float32), jnp.zeros((PAIRS,), jnp.float32))
    (column_peak, column_total), (row_peaks, row_totals) = lax.scan(stats_step, start_pair, text_blocks)

    def grad_step(image_acc, inputs):
        text_block, row_peak, row_total, block_id = inputs
        scores = logit_mult * jnp.dot(text_block, image_low.T, preferred_element_type=jnp.float32)
        text_ids = (block_id * PAIRS_DEV + jnp.arange(PAIRS_DEV, dtype=jnp.int32)).astype(jnp.int32)
        positive = (text_ids[:, None] == column_ids[None, :]).astype(jnp.float32)
        row_prob = jnp.exp(scores - row_peak[:, None]) / row_total[:, None]
        column_prob = jnp.exp(scores - column_peak[None, :]) / column_total[None, :]
        score_grad = (0.5 * (row_prob + column_prob) - positive).astype(jnp.bfloat16)
        text_part = logit_mult * jnp.dot(score_grad, image_low, preferred_element_type=jnp.float32)
        image_acc = image_acc + logit_mult * jnp.dot(score_grad.T, text_block, preferred_element_type=jnp.float32)
        return (image_acc, text_part)
    image_unit_grad, text_parts = lax.scan(grad_step, jnp.zeros((PAIRS, D), jnp.float32), (text_blocks, row_peaks, row_totals, block_ids))
    text_unit_grad = text_parts.reshape(PAIRS, D)
    top_grad = unit_backward(text_unit, text_length, text_unit_grad).astype(jnp.bfloat16)
    image_grad = unit_backward(image_unit, image_length, image_unit_grad).astype(jnp.bfloat16)
    layer_grad = top_grad
    first_grads = []
    second_grads = []
    for layer in reversed(range(LAYERS)):
        inputs_now = layer_inputs[layer]
        pre_act = jnp.dot(inputs_now, w_in[layer], preferred_element_type=jnp.float32)
        activation = quick_gelu(pre_act).astype(jnp.bfloat16)
        back_grad = jnp.dot(layer_grad, w_out[layer].T, preferred_element_type=jnp.float32)
        pre_grad = (back_grad * quick_slope(pre_act)).astype(jnp.bfloat16)
        first_grads.insert(0, jnp.dot(inputs_now.T, pre_grad, preferred_element_type=jnp.float32))
        second_grads.insert(0, jnp.dot(layer_grad.T, activation, preferred_element_type=jnp.float32))
        layer_grad = (layer_grad.astype(jnp.float32) + jnp.dot(pre_grad, w_in[layer].T, preferred_element_type=jnp.float32)).astype(jnp.bfloat16)
    return (image_grad, layer_grad, jnp.stack(first_grads), jnp.stack(second_grads))
```

```python
import functools

import jax
import jax.numpy as jnp
from jax import lax
from jax.experimental import pallas as pl
from jax.experimental.pallas import tpu as pltpu
from jax.sharding import PartitionSpec as P

MESH = pl.DeviceIdType.MESH
F32 = jnp.float32
BF16 = jnp.bfloat16
LOW = -1e30


def dot_nt(a, b):
    return lax.dot_general(a, b, (((1,), (1,)), ((), ())), preferred_element_type=F32)


def dot_nn(a, b):
    return lax.dot_general(a, b, (((1,), (0,)), ((), ())), preferred_element_type=F32)


def dot_tn(a, b):
    return lax.dot_general(a, b, (((0,), (0,)), ((), ())), preferred_element_type=F32)


def unit_rows(values):
    wide = values.astype(F32)
    length = jnp.sqrt(jnp.sum(wide * wide, axis=1, keepdims=True) + 1.0)
    return wide / length, length


def unit_backward(unit, length, grad):
    return (grad - unit * jnp.sum(unit * grad, axis=1, keepdims=True)) / length


def slope_of(pre):
    s = jax.nn.sigmoid(1.702 * pre)
    return s + 1.702 * pre * s * (1.0 - s)


def rows(start, size=128):
    return pl.ds(pl.multiple_of(start, 128), size)


def copy_to(src, dst, send, recv, device):
    return pltpu.make_async_remote_copy(
        src_ref=src, dst_ref=dst, send_sem=send, recv_sem=recv, device_id=device, device_id_type=MESH
    )


def loop(count, fn, start=0):
    def step(i, _):
        fn(i)
        return 0

    lax.fori_loop(start, count, step, 0)


def kernel(
    scale, text, image, hin, win, wout,
    image_out, input_out, first_out, second_out,
    cols, tlow, tlow_t, scores, grads, row_m, row_s, row_a,
    rst, rst_in, rst_a, cst, cst_in, col_b,
    tshare, tshare_in, ishare, ishare_in, ihalf,
    wi_all, wo_all, hother, act, slope, slope_own, hin_t, gbuf, gin, gown, inbuf,
    wg1, wg1_in, wg2, wg2_in,
    cols_ss, cols_rs, wt_ss, wt_rs, h_s, rst_ss, rst_rs, cst_ss, cst_rs,
    ts_ss, ts_rs, is_ss, is_rs, ih_s, g1_ss, g0_ss, g_rs, in_ss, in_rs,
    w1_ss, w1_rs, w2_ss, w2_rs,
):
    section = lax.axis_index("section")
    dp = lax.axis_index("dp")
    mp = lax.axis_index("mp")
    me = section * 4 + mp
    x, core = me // 2, me % 2
    z, y = dp // 4, dp % 4
    mult = scale[0]

    def line(q):
        return {"section": q // 4, "mp": q % 4}

    def plane(k):
        return ((z + k // 4) % 4) * 4 + (y + k % 4) % 4

    def mirror(k):
        return ((4 - k // 4) % 4) * 4 + (4 - k % 4) % 4

    barrier = pltpu.get_barrier_semaphore()

    def greet_plane(k):
        pl.semaphore_signal(barrier, inc=1, device_id={"dp": plane(k)}, device_id_type=MESH)

    def greet_line(i):
        pl.semaphore_signal(barrier, inc=1, device_id=line((me + i) % 8), device_id_type=MESH)

    loop(16, greet_plane, 1)
    loop(8, greet_line, 1)

    own_half = image[pl.ds(pl.multiple_of(section * 128, 128), 128), :]
    image_unit, image_len = unit_rows(own_half)
    cols[0] = image_unit.astype(BF16)

    pl.semaphore_wait(barrier, 22)

    def cols_copy(k):
        return copy_to(cols.at[0], cols.at[mirror(k)], cols_ss.at[k], cols_rs.at[mirror(k)], {"dp": plane(k)})

    def cols_wait(k):
        copy_to(cols.at[k], cols.at[k], cols_ss.at[k], cols_rs.at[k], {"dp": dp}).wait_recv()

    loop(16, lambda k: cols_copy(k).start(), 1)

    right, left, opposite = (x + 1) % 4, (x + 3) % 4, (x + 2) % 4
    weights = (wi_all, wo_all)

    def weight_copy(n, origin, which, to, src=None):
        block = weights[which].at[origin]
        return copy_to(block if src is None else src, block, wt_ss.at[n], wt_rs.at[2 * origin + which], line(to))

    def weight_wait(origin, which):
        block = weights[which].at[origin]
        copy_to(block, block, wt_ss.at[0], wt_rs.at[2 * origin + which], line(me)).wait_recv()

    own_w = (win.at[0], wout.at[0])
    weight_plan = [
        (me, 0, right * 2 + core, own_w[0]),
        (me, 1, left * 2 + core, own_w[1]),
        (me, 1, right * 2 + core, own_w[1]),
        (me, 0, left * 2 + core, own_w[0]),
        (me, 0, x * 2 + 1 - core, own_w[0]),
        (me, 1, x * 2 + 1 - core, own_w[1]),
        (left * 2 + core, 0, right * 2 + core, None),
        (right * 2 + core, 1, left * 2 + core, None),
        (left * 2 + core, 0, x * 2 + 1 - core, None),
        (right * 2 + core, 1, x * 2 + 1 - core, None),
        (left * 2 + core, 1, x * 2 + 1 - core, None),
        (right * 2 + core, 0, x * 2 + 1 - core, None),
        (opposite * 2 + core, 0, x * 2 + 1 - core, None),
        (opposite * 2 + core, 1, x * 2 + 1 - core, None),
    ]

    def weight_send(n):
        origin, which, to, src = weight_plan[n]
        return weight_copy(n, origin, which, to, src)

    twin = (1 - section) * 4 + mp
    h_copy = copy_to(hin.at[0, rows(twin * 128), :], hother, h_s.at[0], h_s.at[1], line(twin))
    h_copy.start()
    for n in range(6):
        weight_send(n).start()

    def text_block(r):
        unit, _ = unit_rows(text[rows(r * 128), :])
        low = unit.astype(BF16)
        tlow[rows(r * 128), :] = low
        tlow_t[:, rows(r * 128)] = low.astype(F32).T.astype(BF16)
        row_m[rows(r * 128), :] = jnp.full((128, 128), LOW, F32)
        row_s[rows(r * 128), :] = jnp.zeros((128, 128), F32)

    loop(8, text_block)

    def score_pair(p):
        for j in (0, 1):
            pl.when(2 * p + j > 0)(functools.partial(cols_wait, 2 * p + j))
        pair = cols[pl.ds(2 * p, 2)].reshape(256, 512)
        scores[p] = dot_nt(tlow[...], pair) * mult

        def block(r, carry):
            c_m, c_s = carry
            s = scores[p, rows(r * 128), :]
            s3 = s.reshape(16, 8, 256)
            n_m = jnp.maximum(c_m, jnp.max(s3, axis=0))
            c_s = c_s * jnp.exp(c_m - n_m) + jnp.sum(jnp.exp(s3 - n_m[None]), axis=0)
            old = row_m[rows(r * 128), :]
            s0, s1 = s[:, :128], s[:, 128:]
            new = jnp.maximum(old, jnp.maximum(s0, s1))
            row_s[rows(r * 128), :] = (
                row_s[rows(r * 128), :] * jnp.exp(old - new) + jnp.exp(s0 - new) + jnp.exp(s1 - new)
            )
            row_m[rows(r * 128), :] = new
            return n_m, c_s

        c_m, c_s = lax.fori_loop(
            0, 8, block, (jnp.full((8, 256), LOW, F32), jnp.zeros((8, 256), F32))
        )
        peak = jnp.max(c_m, axis=0, keepdims=True)
        total = jnp.sum(c_s * jnp.exp(c_m - peak), axis=0, keepdims=True)
        for j in (0, 1):
            at = pl.ds(plane(2 * p + j), 1)
            cst[0, at, :] = peak[:, j * 128 : (j + 1) * 128]
            cst[1, at, :] = total[:, j * 128 : (j + 1) * 128]

    loop(8, score_pair)

    def cst_copy(k):
        return copy_to(cst, cst_in.at[dp], cst_ss.at[k], cst_rs.at[dp], {"dp": plane(k)})

    def cst_wait(k):
        copy_to(cst, cst_in.at[plane(k)], cst_ss.at[k], cst_rs.at[plane(k)], {"dp": dp}).wait_recv()

    loop(16, lambda k: cst_copy(k).start(), 1)
    cst_in[dp] = cst[...]

    for r in range(8):
        m_t = row_m[r * 128 : (r + 1) * 128, :].T
        s_t = row_s[r * 128 : (r + 1) * 128, :].T
        peak = jnp.max(m_t, axis=0, keepdims=True)
        rst[0, r : r + 1, :] = peak
        rst[1, r : r + 1, :] = jnp.sum(s_t * jnp.exp(m_t - peak), axis=0, keepdims=True)

    def rst_copy(i):
        q = (me + i) % 8
        return copy_to(rst, rst_in.at[me], rst_ss.at[i], rst_rs.at[me], line(q))

    def rst_wait(i):
        q = (me + i) % 8
        copy_to(rst, rst_in.at[q], rst_ss.at[i], rst_rs.at[q], line(me)).wait_recv()

    loop(8, lambda i: rst_copy(i).start(), 1)
    rst_in[me] = rst[...]

    weight_wait(left * 2 + core, 0)
    weight_send(6).start()
    weight_wait(right * 2 + core, 1)
    weight_send(7).start()
    weight_send(8).start()
    weight_send(9).start()

    def hidden_block(r):
        at = rows(r * 128)
        h = hin[0, at, :]
        pre = dot_nn(h, win[0])
        sig = jax.nn.sigmoid(1.702 * pre)
        act[at, :] = (pre * sig).astype(BF16)
        slope[at, :] = sig + 1.702 * pre * sig * (1.0 - sig)
        hin_t[:, at] = h.astype(F32).T.astype(BF16)

    loop(8, hidden_block)

    loop(8, rst_wait, 1)
    peak = jnp.max(rst_in[:, 0], axis=0)
    total = jnp.sum(rst_in[:, 1] * jnp.exp(rst_in[:, 0] - peak[None]), axis=0)
    rst_a[...] = peak + jnp.log(2.0 * total)
    for r in range(8):
        row_a[r * 128 : (r + 1) * 128, :] = jnp.broadcast_to(rst_a[r : r + 1, :], (128, 128)).T

    loop(16, cst_wait, 1)
    peak = jnp.max(cst_in[:, 0], axis=0)
    total = jnp.sum(cst_in[:, 1] * jnp.exp(cst_in[:, 0] - peak[None]), axis=0)
    col_b[...] = peak + jnp.log(2.0 * total)

    weight_wait(left * 2 + core, 1)
    weight_send(10).start()
    weight_wait(right * 2 + core, 0)
    weight_send(11).start()

    def prob(s, at, b):
        return jnp.exp(s - row_a[at, :]) + jnp.exp(s - b)

    def tshare_copy(q):
        return copy_to(tshare.at[q], tshare_in.at[me], ts_ss.at[q], ts_rs.at[me], line(q))

    def text_part(i):
        chip = (x + 1 + i) % 4

        def grad_block(t):
            p = t % 8
            at = rows(chip * 256 + (t // 8) * 128)
            for j in (0, 1):
                s = scores[p, at, j * 128 : (j + 1) * 128]
                b = col_b[pl.ds(plane(2 * p + j), 1), :]
                grads[at, pl.ds(pl.multiple_of(p * 256 + j * 128, 128), 128)] = prob(s, at, b).astype(BF16)

        loop(16, grad_block)

        mine = 2 * mp + section

        @pl.when(mine // 2 == chip)
        def _():
            at = rows(mine * 128)
            s = scores[0, at, :128]
            eye = lax.broadcasted_iota(jnp.int32, (128, 128), 0) == lax.broadcasted_iota(jnp.int32, (128, 128), 1)
            part = prob(s, at, col_b[pl.ds(dp, 1), :])
            grads[at, :128] = (part - jnp.where(eye, 1.0, 0.0)).astype(BF16)

        part = dot_nn(grads[rows(chip * 256, 256), :], cols[...].reshape(2048, 512))
        for j in (0, 1):
            q = chip * 2 + j
            tshare[q] = part[j * 128 : (j + 1) * 128].astype(BF16)
            pl.when(q != me)(lambda q=q: tshare_copy(q).start())

    loop(4, text_part)

    def ishare_copy(k):
        return copy_to(ishare.at[k], ishare_in.at[mirror(k)], is_ss.at[k], is_rs.at[mirror(k)], {"dp": plane(k)})

    def image_part(p):
        part = dot_nn(tlow_t[...], grads[:, pl.ds(pl.multiple_of(p * 256, 256), 256)])
        for j in (0, 1):
            k = 2 * p + j
            ishare[k] = part[:, j * 128 : (j + 1) * 128].astype(BF16)
            pl.when(k > 0)(lambda k=k: ishare_copy(k).start())

    loop(8, image_part)

    weight_wait(opposite * 2 + core, 0)
    weight_send(12).start()
    weight_wait(opposite * 2 + core, 1)
    weight_send(13).start()

    h_copy.wait_recv()

    def own_block(r):
        def other_wait():
            for which in (0, 1):
                weight_wait(r, which)

        pl.when(r % 2 != core)(other_wait)

        @pl.when(r == me)
        def _():
            wi_all[r] = win[0]
            wo_all[r] = wout[0]

        h = jnp.where(r // 4 == section, hin[0, rows(me * 128), :], hother[...])
        slope_own[r] = slope_of(dot_nn(h, wi_all[r]))

    loop(8, own_block)

    def tshare_sum(i, acc):
        q = (me + i) % 8
        copy_to(tshare.at[q], tshare_in.at[q], ts_ss.at[q], ts_rs.at[q], line(me)).wait_recv()
        return acc + tshare_in[q].astype(F32)

    total = lax.fori_loop(1, 8, tshare_sum, tshare[me].astype(F32)) * mult
    unit, length = unit_rows(text[rows(me * 128), :])
    gown[0] = unit_backward(unit, length, total).astype(BF16)

    def g_copy(layer, m, sems):
        return copy_to(gown.at[1 - layer], gbuf.at[me], sems.at[m], g_rs.at[me], {"section": layer, "mp": m})

    def g_send(layer, sems):
        for m in range(4):
            pl.when(me != layer * 4 + m)(lambda m=m: g_copy(layer, m, sems).start())

        @pl.when(section == layer)
        def _():
            gbuf[me] = gown[1 - layer]

    def chain(layer):
        g = gown[1 - layer]

        def step(j, acc):
            q = layer * 4 + j
            back = dot_nt(g, wo_all[q])
            pre_grad = (back * slope_own[q]).astype(BF16)
            return acc + dot_nt(pre_grad, wi_all[q])

        return lax.fori_loop(0, 4, step, g.astype(F32)).astype(BF16)

    g_send(1, g1_ss)
    gown[1] = chain(1)
    g_send(0, g0_ss)
    lowest = chain(0)
    gin[0] = lowest[:, :256]
    gin[1] = lowest[:, 256:]

    def in_copy(i):
        q = (me + i) % 8
        return copy_to(gin.at[q // 4], inbuf.at[me], in_ss.at[i], in_rs.at[me], line(q))

    loop(8, lambda i: in_copy(i).start(), 1)
    inbuf[me] = gin[section]

    def g_wait(i):
        q = (me + i) % 8
        copy_to(gbuf.at[q], gbuf.at[q], g1_ss.at[0], g_rs.at[q], line(me)).wait_recv()

    loop(8, g_wait, 1)

    full = gbuf[...].reshape(1024, 512)

    def wg_copy(buf, landed, ss, rs, k):
        return copy_to(buf.at[plane(k)], landed.at[dp], ss.at[k], rs.at[dp], {"dp": plane(k)})

    wg2[...] = dot_tn(full, act[...]).reshape(16, 32, 512).astype(BF16)
    loop(16, lambda k: wg_copy(wg2, wg2_in, w2_ss, w2_rs, k).start(), 1)

    def back_block(r):
        at = rows(r * 128)
        back = dot_nt(gbuf[r], wout[0])
        act[at, :] = (back * slope[at, :]).astype(BF16)

    loop(8, back_block)
    wg1[...] = dot_nn(hin_t[...], act[...]).reshape(16, 32, 512).astype(BF16)
    loop(16, lambda k: wg_copy(wg1, wg1_in, w1_ss, w1_rs, k).start(), 1)

    def ishare_sum(k, acc):
        copy_to(ishare.at[k], ishare_in.at[k], is_ss.at[k], is_rs.at[k], {"dp": dp}).wait_recv()
        return acc + ishare_in[k].astype(F32)

    total = lax.fori_loop(1, 16, ishare_sum, ishare[0].astype(F32)).T * mult
    own_half = image[pl.ds(pl.multiple_of(section * 128, 128), 128), :]
    image_unit, image_len = unit_rows(own_half)
    ihalf[0] = unit_backward(image_unit, image_len, total).astype(BF16)
    ihalf_copy = copy_to(ihalf.at[0], ihalf.at[1], ih_s.at[0], ih_s.at[1], line(twin))
    ihalf_copy.start()

    def in_wait(i):
        q = (me + i) % 8
        copy_to(gin.at[0], inbuf.at[q], in_ss.at[i], in_rs.at[q], line(me)).wait_recv()

    loop(8, in_wait, 1)
    input_out[...] = inbuf[...].reshape(1024, 256)

    def wg_sum(buf, landed, ss, rs, out):
        def step(k, acc):
            copy_to(buf.at[0], landed.at[plane(k)], ss.at[k], rs.at[plane(k)], {"dp": dp}).wait_recv()
            return acc + landed[plane(k)].astype(F32)

        out[0] = lax.fori_loop(1, 16, step, buf[dp].astype(F32))

    image_out[rows(section * 128), :] = ihalf[0]
    ihalf_copy.wait_recv()
    image_out[rows((1 - section) * 128), :] = ihalf[1]
    wg_sum(wg2, wg2_in, w2_ss, w2_rs, second_out)
    wg_sum(wg1, wg1_in, w1_ss, w1_rs, first_out)

    loop(16, lambda k: cols_copy(k).wait_send(), 1)
    h_copy.wait_send()
    for n in range(14):
        weight_send(n).wait_send()
    loop(16, lambda k: cst_copy(k).wait_send(), 1)
    loop(8, lambda i: rst_copy(i).wait_send(), 1)
    loop(8, lambda i: tshare_copy((me + i) % 8).wait_send(), 1)
    loop(16, lambda k: ishare_copy(k).wait_send(), 1)
    ihalf_copy.wait_send()
    for layer, sems in ((1, g1_ss), (0, g0_ss)):
        for m in range(4):
            pl.when(me != layer * 4 + m)(lambda m=m, layer=layer, sems=sems: g_copy(layer, m, sems).wait_send())
    loop(8, lambda i: in_copy(i).wait_send(), 1)
    loop(16, lambda k: wg_copy(wg2, wg2_in, w2_ss, w2_rs, k).wait_send(), 1)
    loop(16, lambda k: wg_copy(wg1, wg1_in, w1_ss, w1_rs, k).wait_send(), 1)


def body(text_feats, image_feats, logit_scale, layer_inputs, w_in, w_out):
    vmem = pl.BlockSpec(memory_space=pltpu.VMEM)
    dma = pltpu.SemaphoreType.DMA
    scratch = [
        pltpu.VMEM((16, 128, 512), BF16),
        pltpu.VMEM((1024, 512), BF16),
        pltpu.VMEM((512, 1024), BF16),
        pltpu.VMEM((8, 1024, 256), F32),
        pltpu.VMEM((1024, 2048), BF16),
        pltpu.VMEM((1024, 128), F32),
        pltpu.VMEM((1024, 128), F32),
        pltpu.VMEM((1024, 128), F32),
        pltpu.VMEM((2, 8, 128), F32),
        pltpu.VMEM((8, 2, 8, 128), F32),
        pltpu.VMEM((8, 128), F32),
        pltpu.VMEM((2, 16, 128), F32),
        pltpu.VMEM((16, 2, 16, 128), F32),
        pltpu.VMEM((16, 128), F32),
        pltpu.VMEM((8, 128, 512), BF16),
        pltpu.VMEM((8, 128, 512), BF16),
        pltpu.VMEM((16, 512, 128), BF16),
        pltpu.VMEM((16, 512, 128), BF16),
        pltpu.VMEM((2, 128, 512), BF16),
        pltpu.VMEM((8, 512, 512), BF16),
        pltpu.VMEM((8, 512, 512), BF16),
        pltpu.VMEM((128, 512), BF16),
        pltpu.VMEM((1024, 512), BF16),
        pltpu.VMEM((1024, 512), F32),
        pltpu.VMEM((8, 128, 512), F32),
        pltpu.VMEM((512, 1024), BF16),
        pltpu.VMEM((8, 128, 512), BF16),
        pltpu.VMEM((2, 128, 256), BF16),
        pltpu.VMEM((2, 128, 512), BF16),
        pltpu.VMEM((8, 128, 256), BF16),
        pltpu.VMEM((16, 32, 512), BF16),
        pltpu.VMEM((16, 32, 512), BF16),
        pltpu.VMEM((16, 32, 512), BF16),
        pltpu.VMEM((16, 32, 512), BF16),
        dma((16,)), dma((16,)),
        dma((14,)), dma((16,)),
        dma((2,)),
        dma((8,)), dma((8,)),
        dma((16,)), dma((16,)),
        dma((8,)), dma((8,)),
        dma((16,)), dma((16,)),
        dma((2,)),
        dma((4,)), dma((4,)), dma((8,)),
        dma((8,)), dma((8,)),
        dma((16,)), dma((16,)), dma((16,)), dma((16,)),
    ]
    return pl.pallas_call(
        kernel,
        out_shape=(
            jax.ShapeDtypeStruct((256, 512), BF16),
            jax.ShapeDtypeStruct((1024, 256), BF16),
            jax.ShapeDtypeStruct((1, 32, 512), F32),
            jax.ShapeDtypeStruct((1, 32, 512), F32),
        ),
        in_specs=[pl.BlockSpec(memory_space=pltpu.SMEM)] + [vmem] * 5,
        out_specs=(vmem,) * 4,
        scratch_shapes=scratch,
        compiler_params=pltpu.CompilerParams(
            collective_id=0, has_side_effects=True, vmem_limit_bytes=62 * 1024 * 1024
        ),
    )(logit_scale, text_feats, image_feats, layer_inputs, w_in, w_out)


def solution(mesh):
    placed = (
        P("dp", None),
        P(("dp", "mp"), None),
        P(),
        P("section", "dp", None),
        P("section", None, "mp"),
        P("section", "mp", None),
    )
    return jax.shard_map(
        body,
        mesh=mesh,
        in_specs=placed,
        out_specs=(
            P(("dp", "mp"), None),
            P("dp", "section"),
            P("section", "dp", "mp"),
            P("section", "dp", "mp"),
        ),
        check_vma=False,
    )
```

```python
import functools

import jax
import jax.numpy as jnp
from jax import lax
from jax.experimental import pallas as pl
from jax.experimental.pallas import tpu as pltpu
from jax.sharding import PartitionSpec as P

MESH = pl.DeviceIdType.MESH
F32 = jnp.float32
BF16 = jnp.bfloat16
LOW = -1e30
ORDER = (
    (0, 0), (0, 1), (0, 3), (1, 0), (3, 0), (1, 1), (1, 3), (3, 1),
    (3, 3), (0, 2), (2, 0), (1, 2), (3, 2), (2, 1), (2, 3), (2, 2),
)


def dot_nt(a, b):
    return lax.dot_general(a, b, (((1,), (1,)), ((), ())), preferred_element_type=F32)


def dot_nn(a, b):
    return lax.dot_general(a, b, (((1,), (0,)), ((), ())), preferred_element_type=F32)


def dot_tn(a, b):
    return lax.dot_general(a, b, (((0,), (0,)), ((), ())), preferred_element_type=F32)


def unit_rows(values):
    wide = values.astype(F32)
    length = jnp.sqrt(jnp.sum(wide * wide, axis=1, keepdims=True) + 1.0)
    return wide / length, length


def unit_backward(unit, length, grad):
    return (grad - unit * jnp.sum(unit * grad, axis=1, keepdims=True)) / length


def slope_of(pre):
    s = jax.nn.sigmoid(1.702 * pre)
    return s + 1.702 * pre * s * (1.0 - s)


def rows(start, size=128):
    return pl.ds(pl.multiple_of(start, 128), size)


def copy_to(src, dst, send, recv, device):
    return pltpu.make_async_remote_copy(
        src_ref=src, dst_ref=dst, send_sem=send, recv_sem=recv, device_id=device, device_id_type=MESH
    )


def loop(count, fn, start=0):
    def step(i, _):
        fn(i)
        return 0

    lax.fori_loop(start, count, step, 0)


def kernel(
    scale, text, image, hin, win, wout,
    image_out, input_out, first_out, second_out,
    cols, tlow, tlow_t, scores, grads, row_m, row_s, row_a,
    rst, rst_in, rst_a, own_stat, cst, cst_in, col_b,
    tshare, tpass, tshare_in, ishare, ifar_in, isum, inear_in, ifull, ihalf,
    wi_all, wo_all, hother, act, slope, slope_own, hin_t, gbuf, gin, gown, inbuf,
    wg1, wg1_in, wg2, wg2_in,
    cols_ss, cols_rs, wt_ss, wt_rs, h_s, rst_ss, rst_rs, cst_ss, cst_rs,
    tp_ss, tp_rs, ts_ss, ts_rs, if_ss, if_rs, ir_ss, ir_rs, ih_s,
    g1_ss, g0_ss, gp_ss, g_rs, in_ss, in_rs,
    w1_ss, w1_rs, w2_ss, w2_rs,
):
    section = lax.axis_index("section")
    dp = lax.axis_index("dp")
    mp = lax.axis_index("mp")
    me = section * 4 + mp
    x, core = me // 2, me % 2
    z, y = dp // 4, dp % 4
    mult = scale[0]

    def line(q):
        return {"section": q // 4, "mp": q % 4}

    def plane(dz, dy):
        return ((z + dz) % 4) * 4 + (y + dy) % 4

    def slot(dz, dy):
        return ORDER.index((dz % 4, dy % 4))

    def away(k):
        return plane(k // 4, k % 4)

    sends = []

    barrier = pltpu.get_barrier_semaphore()

    def greet_plane(k):
        pl.semaphore_signal(barrier, inc=1, device_id={"dp": away(k)}, device_id_type=MESH)

    def greet_line(i):
        pl.semaphore_signal(barrier, inc=1, device_id=line((me + i) % 8), device_id_type=MESH)

    loop(16, greet_plane, 1)
    loop(8, greet_line, 1)

    own_half = image[pl.ds(pl.multiple_of(section * 128, 128), 128), :]
    image_unit, image_len = unit_rows(own_half)
    cols[0] = image_unit.astype(BF16)

    def text_block(r):
        unit, _ = unit_rows(text[rows(r * 128), :])
        low = unit.astype(BF16)
        tlow[rows(r * 128), :] = low
        tlow_t[:, rows(r * 128)] = low.astype(F32).T.astype(BF16)
        row_m[rows(r * 128), :] = jnp.full((128, 128), LOW, F32)
        row_s[rows(r * 128), :] = jnp.zeros((128, 128), F32)

    loop(8, text_block)
    pl.semaphore_wait(barrier, 22)

    def ag_send(dz, dy, lo, size, ez, ey):
        there = slot(dz - ez, dy - ey)
        copy = copy_to(
            cols.at[slot(dz, dy), lo : lo + size],
            cols.at[there, lo : lo + size],
            cols_ss.at[len(sends)],
            cols_rs.at[there * 4 + lo // 32],
            {"dp": plane(ez, ey)},
        )
        copy.start()
        sends.append(copy)

    def ag_wait(dz, dy, lo, size):
        here = slot(dz, dy)
        block = cols.at[here, lo : lo + size]
        copy_to(block, block, cols_ss.at[0], cols_rs.at[here * 4 + lo // 32], {"dp": dp}).wait_recv()

    def flip(swap, *pair):
        return pair[::-1] if swap else pair

    def half_send(swap, first, second, to_first, to_second, lo=0, size=64):
        dz, dy = flip(swap, first, second)
        ez, ey = flip(swap, to_first, to_second)
        ag_send(dz, dy, lo + 64 * swap, size, ez, ey)

    def half_wait(swap, first, second, lo=0, size=64):
        dz, dy = flip(swap, first, second)
        ag_wait(dz, dy, lo + 64 * swap, size)

    for to in ((0, 1), (0, 3), (1, 0), (3, 0)):
        for swap in (0, 1):
            half_send(swap, 0, 0, *to)

    right, left, opposite = (x + 1) % 4, (x + 3) % 4, (x + 2) % 4
    weights = (wi_all, wo_all)

    def weight_copy(n, origin, which, to, src=None):
        block = weights[which].at[origin]
        return copy_to(block if src is None else src, block, wt_ss.at[n], wt_rs.at[2 * origin + which], line(to))

    def weight_wait(origin, which):
        block = weights[which].at[origin]
        copy_to(block, block, wt_ss.at[0], wt_rs.at[2 * origin + which], line(me)).wait_recv()

    own_w = (win.at[0], wout.at[0])
    weight_plan = [
        (me, 0, right * 2 + core, own_w[0]),
        (me, 1, left * 2 + core, own_w[1]),
        (me, 1, right * 2 + core, own_w[1]),
        (me, 0, left * 2 + core, own_w[0]),
        (me, 0, x * 2 + 1 - core, own_w[0]),
        (me, 1, x * 2 + 1 - core, own_w[1]),
        (left * 2 + core, 0, right * 2 + core, None),
        (right * 2 + core, 1, left * 2 + core, None),
        (left * 2 + core, 0, x * 2 + 1 - core, None),
        (right * 2 + core, 1, x * 2 + 1 - core, None),
        (left * 2 + core, 1, x * 2 + 1 - core, None),
        (right * 2 + core, 0, x * 2 + 1 - core, None),
        (opposite * 2 + core, 0, x * 2 + 1 - core, None),
        (opposite * 2 + core, 1, x * 2 + 1 - core, None),
    ]

    def weight_send(n):
        origin, which, to, src = weight_plan[n]
        return weight_copy(n, origin, which, to, src)

    twin = (1 - section) * 4 + mp
    h_copy = copy_to(hin.at[0, rows(twin * 128), :], hother, h_s.at[0], h_s.at[1], line(twin))
    h_copy.start()
    for n in range(6):
        weight_send(n).start()

    def score_pair(p):
        pair = cols[pl.ds(2 * p, 2)].reshape(256, 512)
        scores[p] = dot_nt(tlow[...], pair) * mult

        def block(r, carry):
            c_m, c_s = carry
            s = scores[p, rows(r * 128), :]
            s3 = s.reshape(16, 8, 256)
            n_m = jnp.maximum(c_m, jnp.max(s3, axis=0))
            c_s = c_s * jnp.exp(c_m - n_m) + jnp.sum(jnp.exp(s3 - n_m[None]), axis=0)
            old = row_m[rows(r * 128), :]
            s0, s1 = s[:, :128], s[:, 128:]
            new = jnp.maximum(old, jnp.maximum(s0, s1))
            row_s[rows(r * 128), :] = (
                row_s[rows(r * 128), :] * jnp.exp(old - new) + jnp.exp(s0 - new) + jnp.exp(s1 - new)
            )
            row_m[rows(r * 128), :] = new
            return n_m, c_s

        c_m, c_s = lax.fori_loop(
            0, 8, block, (jnp.full((8, 256), LOW, F32), jnp.zeros((8, 256), F32))
        )
        peak = jnp.max(c_m, axis=0, keepdims=True)
        total = jnp.sum(c_s * jnp.exp(c_m - peak), axis=0, keepdims=True)
        for j in (0, 1):
            own_stat[0, pl.ds(2 * p + j, 1), :] = peak[:, j * 128 : (j + 1) * 128]
            own_stat[1, pl.ds(2 * p + j, 1), :] = total[:, j * 128 : (j + 1) * 128]

    def spread(swap, first, second):
        for to in (1, 3):
            half_send(swap, first, second, to, 0)

    both = (0, 1)
    for swap in both:
        half_wait(swap, 0, 1)
        half_wait(swap, 0, 3)
        half_send(swap, 0, 1, 0, 3, 0, 32)
        half_send(swap, 0, 3, 0, 1, 32, 32)
    for swap in both:
        spread(swap, 0, 1)
        spread(swap, 0, 3)
    for swap in both:
        half_wait(swap, 1, 0)
        half_send(swap, 1, 0, 3, 0)
        half_wait(swap, 3, 0)
    for swap in both:
        half_wait(swap, 0, 2, 0, 32)
        half_wait(swap, 0, 2, 32, 32)
        spread(swap, 0, 2)
    loop(2, score_pair)
    for swap in both:
        for second in (1, 3):
            half_wait(swap, 3, second)
            half_send(swap, 3, second, 1, 0)
            half_wait(swap, 1, second)
        half_wait(swap, 2, 0)
    loop(5, score_pair, 2)
    for swap in both:
        half_wait(swap, 1, 2)
        half_send(swap, 1, 2, 3, 0)
        half_wait(swap, 3, 2)
    for swap in both:
        half_wait(swap, 2, 1)
        half_wait(swap, 2, 3)
    loop(7, score_pair, 5)
    for swap in both:
        half_wait(swap, 2, 2)
    score_pair(7)
    for k, (dz, dy) in enumerate(ORDER):
        cst[:, pl.ds(plane(dz, dy), 1), :] = own_stat[:, k : k + 1, :]

    def cst_copy(k):
        return copy_to(cst, cst_in.at[dp], cst_ss.at[k], cst_rs.at[dp], {"dp": away(k)})

    def cst_wait(k):
        copy_to(cst, cst_in.at[away(k)], cst_ss.at[k], cst_rs.at[away(k)], {"dp": dp}).wait_recv()

    loop(16, lambda k: cst_copy(k).start(), 1)
    cst_in[dp] = cst[...]

    for r in range(8):
        m_t = row_m[r * 128 : (r + 1) * 128, :].T
        s_t = row_s[r * 128 : (r + 1) * 128, :].T
        peak = jnp.max(m_t, axis=0, keepdims=True)
        rst[0, r : r + 1, :] = peak
        rst[1, r : r + 1, :] = jnp.sum(s_t * jnp.exp(m_t - peak), axis=0, keepdims=True)

    def rst_copy(i):
        q = (me + i) % 8
        return copy_to(rst, rst_in.at[me], rst_ss.at[i], rst_rs.at[me], line(q))

    def rst_wait(i):
        q = (me + i) % 8
        copy_to(rst, rst_in.at[q], rst_ss.at[i], rst_rs.at[q], line(me)).wait_recv()

    loop(8, lambda i: rst_copy(i).start(), 1)
    rst_in[me] = rst[...]

    weight_wait(left * 2 + core, 0)
    weight_send(6).start()
    weight_wait(right * 2 + core, 1)
    weight_send(7).start()
    weight_send(8).start()
    weight_send(9).start()

    def hidden_block(r):
        at = rows(r * 128)
        h = hin[0, at, :]
        pre = dot_nn(h, win[0])
        sig = jax.nn.sigmoid(1.702 * pre)
        act[at, :] = (pre * sig).astype(BF16)
        slope[at, :] = sig + 1.702 * pre * sig * (1.0 - sig)
        hin_t[:, at] = h.astype(F32).T.astype(BF16)

    loop(8, hidden_block)

    loop(8, rst_wait, 1)
    peak = jnp.max(rst_in[:, 0], axis=0)
    total = jnp.sum(rst_in[:, 1] * jnp.exp(rst_in[:, 0] - peak[None]), axis=0)
    rst_a[...] = peak + jnp.log(2.0 * total)
    for r in range(8):
        row_a[r * 128 : (r + 1) * 128, :] = jnp.broadcast_to(rst_a[r : r + 1, :], (128, 128)).T

    loop(16, cst_wait, 1)
    peak = jnp.max(cst_in[:, 0], axis=0)
    total = jnp.sum(cst_in[:, 1] * jnp.exp(cst_in[:, 0] - peak[None]), axis=0)
    cst_in[dp, 0] = peak + jnp.log(2.0 * total)
    for k, (dz, dy) in enumerate(ORDER):
        col_b[k : k + 1, :] = cst_in[dp, 0, pl.ds(plane(dz, dy), 1), :]

    weight_wait(left * 2 + core, 1)
    weight_send(10).start()
    weight_wait(right * 2 + core, 0)
    weight_send(11).start()

    def prob(s, at, b):
        return jnp.exp(s - row_a[at, :]) + jnp.exp(s - b)

    def pass_copy(chip):
        other = chip * 2 + 1 - core
        return copy_to(tshare.at[other], tpass.at[chip], tp_ss.at[chip], tp_rs.at[chip], line(x * 2 + 1 - core))

    def tshare_copy(chip):
        own = chip * 2 + core
        return copy_to(tshare.at[own], tshare_in.at[x], ts_ss.at[chip], ts_rs.at[x], line(own))

    def text_part(chip):
        def grad_block(t):
            p = t % 8
            at = rows(chip * 256 + (t // 8) * 128)
            for j in (0, 1):
                s = scores[p, at, j * 128 : (j + 1) * 128]
                b = col_b[pl.ds(2 * p + j, 1), :]
                grads[at, pl.ds(pl.multiple_of(p * 256 + j * 128, 128), 128)] = prob(s, at, b).astype(BF16)

        loop(16, grad_block)

        mine = 2 * mp + section

        @pl.when(mine // 2 == chip)
        def _():
            at = rows(mine * 128)
            s = scores[0, at, :128]
            eye = lax.broadcasted_iota(jnp.int32, (128, 128), 0) == lax.broadcasted_iota(jnp.int32, (128, 128), 1)
            part = prob(s, at, col_b[0:1, :])
            grads[at, :128] = (part - jnp.where(eye, 1.0, 0.0)).astype(BF16)

        part = dot_nn(grads[rows(chip * 256, 256), :], cols[...].reshape(2048, 512))
        for j in (0, 1):
            tshare[chip * 2 + j] = part[j * 128 : (j + 1) * 128].astype(BF16)
        pass_copy(chip).start()

    def text_merge(chip):
        own = chip * 2 + core
        pass_copy(chip).wait_recv()
        tshare[own] = (tshare[own].astype(F32) + tpass[chip].astype(F32)).astype(BF16)

    def text_step(i):
        chip = jnp.where(i == 0, opposite, jnp.where(i == 1, right, jnp.where(i == 2, left, x)))
        last = jnp.where(i == 1, opposite, jnp.where(i == 2, right, left))
        text_part(chip)

        @pl.when(i > 0)
        def _():
            text_merge(last)
            tshare_copy(last).start()

    loop(4, text_step)
    text_merge(x)

    def image_part(p):
        part = dot_nn(tlow_t[...], grads[:, p * 256 : (p + 1) * 256])
        for j in (0, 1):
            dz, dy = ORDER[2 * p + j]
            block = part[:, j * 128 : (j + 1) * 128].astype(BF16)
            ishare[0, dz, dy] = block[:256]
            ishare[1, dy, dz] = block[256:]

    def step_of(swap, far):
        return {"dp": plane(*flip(swap, far, 0))}

    def image_far(swap, far):
        n = swap * 3 + 3 - far
        return copy_to(ishare.at[swap, far], ifar_in.at[swap, 3 - far], if_ss.at[n], if_rs.at[n], step_of(swap, far))

    def image_near(swap, far):
        n = swap * 3 + 3 - far
        return copy_to(isum.at[swap, far], inear_in.at[swap, 3 - far], ir_ss.at[n], ir_rs.at[n], step_of(1 - swap, far))

    for p in range(7, -1, -1):
        image_part(p)
    for far in (2, 1, 3):
        for swap in both:
            image_far(swap, far).start()

    weight_wait(opposite * 2 + core, 0)
    weight_send(12).start()
    weight_wait(opposite * 2 + core, 1)
    weight_send(13).start()

    h_copy.wait_recv()

    def own_block(r):
        def other_wait():
            for which in (0, 1):
                weight_wait(r, which)

        pl.when(r % 2 != core)(other_wait)

        @pl.when(r == me)
        def _():
            wi_all[r] = win[0]
            wo_all[r] = wout[0]

        h = jnp.where(r // 4 == section, hin[0, rows(me * 128), :], hother[...])
        slope_own[r] = slope_of(dot_nn(h, wi_all[r]))

    loop(8, own_block)

    def tshare_sum(i, acc):
        chip = (x + i) % 4
        copy_to(tshare.at[0], tshare_in.at[chip], ts_ss.at[chip], ts_rs.at[chip], line(me)).wait_recv()
        return acc + tshare_in[chip].astype(F32)

    total = lax.fori_loop(1, 4, tshare_sum, tshare[me].astype(F32)) * mult
    unit, length = unit_rows(text[rows(me * 128), :])
    gown[0] = unit_backward(unit, length, total).astype(BF16)

    def g_copy(layer, lo, sems):
        to = {"section": layer, "mp": lo * 2 + core}
        return copy_to(gown.at[1 - layer], gbuf.at[me], sems.at[lo], g_rs.at[me], to)

    def g_send(layer, sems):
        for lo in (0, 1):
            pl.when(x != layer * 2 + lo)(lambda lo=lo: g_copy(layer, lo, sems).start())

        @pl.when(section == layer)
        def _():
            gbuf[me] = gown[1 - layer]

    def g_pass(i):
        q = ((x + i) % 4) * 2 + core
        return copy_to(gbuf.at[q], gbuf.at[q], gp_ss.at[i], g_rs.at[q], line(x * 2 + 1 - core))

    def g_arrive(q):
        copy_to(gbuf.at[q], gbuf.at[q], gp_ss.at[0], g_rs.at[q], line(me)).wait_recv()

    def g_relay(i):
        g_arrive(((x + i) % 4) * 2 + core)
        g_pass(i).start()

    def chain(layer):
        g = gown[1 - layer]

        def step(j, acc):
            q = layer * 4 + j
            back = dot_nt(g, wo_all[q])
            pre_grad = (back * slope_own[q]).astype(BF16)
            return acc + dot_nt(pre_grad, wi_all[q])

        return lax.fori_loop(0, 4, step, g.astype(F32)).astype(BF16)

    g_send(1, g1_ss)
    gown[1] = chain(1)
    g_send(0, g0_ss)
    lowest = chain(0)
    gin[0] = lowest[:, :256]
    gin[1] = lowest[:, 256:]

    def in_copy(i):
        q = (me + i) % 8
        return copy_to(gin.at[q // 4], inbuf.at[me], in_ss.at[i], in_rs.at[me], line(q))

    def image_fold(swap):
        total = ishare[swap, 0].astype(F32)
        for far in (1, 2, 3):
            landed = ifar_in.at[swap, far - 1]
            copy_to(landed, landed, if_ss.at[0], if_rs.at[swap * 3 + far - 1], {"dp": dp}).wait_recv()
            total = total + landed[...].astype(F32)
        isum[swap] = total.astype(BF16)
        for far in (2, 1, 3):
            image_near(swap, far).start()

    for swap in both:
        image_fold(swap)
    g_pass(0).start()
    loop(4, g_relay, 1)
    loop(8, lambda i: in_copy(i).start(), 1)
    inbuf[me] = gin[section]
    loop(4, lambda i: g_arrive(((x + i) % 4) * 2 + 1 - core))

    full = gbuf[...].reshape(1024, 512)

    def wg_copy(buf, landed, ss, rs, k):
        return copy_to(buf.at[away(k)], landed.at[dp], ss.at[k], rs.at[dp], {"dp": away(k)})

    wg2[...] = dot_tn(full, act[...]).reshape(16, 32, 512).astype(BF16)
    loop(16, lambda k: wg_copy(wg2, wg2_in, w2_ss, w2_rs, k).start(), 1)

    def back_block(r):
        at = rows(r * 128)
        back = dot_nt(gbuf[r], wout[0])
        act[at, :] = (back * slope[at, :]).astype(BF16)

    loop(8, back_block)
    wg1[...] = dot_nn(hin_t[...], act[...]).reshape(16, 32, 512).astype(BF16)
    loop(16, lambda k: wg_copy(wg1, wg1_in, w1_ss, w1_rs, k).start(), 1)

    for swap in both:
        total = isum[swap, 0].astype(F32)
        for far in (1, 2, 3):
            landed = inear_in.at[swap, far - 1]
            copy_to(landed, landed, ir_ss.at[0], ir_rs.at[swap * 3 + far - 1], {"dp": dp}).wait_recv()
            total = total + landed[...].astype(F32)
        ifull[:, swap * 256 : (swap + 1) * 256] = total.T
    total = ifull[...] * mult
    own_half = image[pl.ds(pl.multiple_of(section * 128, 128), 128), :]
    image_unit, image_len = unit_rows(own_half)
    ihalf[0] = unit_backward(image_unit, image_len, total).astype(BF16)
    ihalf_copy = copy_to(ihalf.at[0], ihalf.at[1], ih_s.at[0], ih_s.at[1], line(twin))
    ihalf_copy.start()

    def in_wait(i):
        q = (me + i) % 8
        copy_to(gin.at[0], inbuf.at[q], in_ss.at[i], in_rs.at[q], line(me)).wait_recv()

    loop(8, in_wait, 1)
    input_out[...] = inbuf[...].reshape(1024, 256)

    def wg_sum(buf, landed, ss, rs, out):
        def step(k, acc):
            copy_to(buf.at[0], landed.at[away(k)], ss.at[k], rs.at[away(k)], {"dp": dp}).wait_recv()
            return acc + landed[away(k)].astype(F32)

        out[0] = lax.fori_loop(1, 16, step, buf[dp].astype(F32))

    image_out[rows(section * 128), :] = ihalf[0]
    ihalf_copy.wait_recv()
    image_out[rows((1 - section) * 128), :] = ihalf[1]
    wg_sum(wg2, wg2_in, w2_ss, w2_rs, second_out)
    wg_sum(wg1, wg1_in, w1_ss, w1_rs, first_out)

    for copy in sends:
        copy.wait_send()
    h_copy.wait_send()
    for n in range(14):
        weight_send(n).wait_send()
    loop(16, lambda k: cst_copy(k).wait_send(), 1)
    loop(8, lambda i: rst_copy(i).wait_send(), 1)
    loop(4, lambda i: pass_copy(i).wait_send())
    loop(4, lambda i: tshare_copy((x + i) % 4).wait_send(), 1)
    for swap in both:
        for far in (1, 2, 3):
            image_far(swap, far).wait_send()
            image_near(swap, far).wait_send()
    ihalf_copy.wait_send()
    for layer, sems in ((1, g1_ss), (0, g0_ss)):
        for lo in (0, 1):
            pl.when(x != layer * 2 + lo)(lambda lo=lo, layer=layer, sems=sems: g_copy(layer, lo, sems).wait_send())
    loop(4, lambda i: g_pass(i).wait_send())
    loop(8, lambda i: in_copy(i).wait_send(), 1)
    loop(16, lambda k: wg_copy(wg2, wg2_in, w2_ss, w2_rs, k).wait_send(), 1)
    loop(16, lambda k: wg_copy(wg1, wg1_in, w1_ss, w1_rs, k).wait_send(), 1)


def body(text_feats, image_feats, logit_scale, layer_inputs, w_in, w_out):
    vmem = pl.BlockSpec(memory_space=pltpu.VMEM)
    dma = pltpu.SemaphoreType.DMA
    scratch = [
        pltpu.VMEM((16, 128, 512), BF16),
        pltpu.VMEM((1024, 512), BF16),
        pltpu.VMEM((512, 1024), BF16),
        pltpu.VMEM((8, 1024, 256), F32),
        pltpu.VMEM((1024, 2048), BF16),
        pltpu.VMEM((1024, 128), F32),
        pltpu.VMEM((1024, 128), F32),
        pltpu.VMEM((1024, 128), F32),
        pltpu.VMEM((2, 8, 128), F32),
        pltpu.VMEM((8, 2, 8, 128), F32),
        pltpu.VMEM((8, 128), F32),
        pltpu.VMEM((2, 16, 128), F32),
        pltpu.VMEM((2, 16, 128), F32),
        pltpu.VMEM((16, 2, 16, 128), F32),
        pltpu.VMEM((16, 128), F32),
        pltpu.VMEM((8, 128, 512), BF16),
        pltpu.VMEM((4, 128, 512), BF16),
        pltpu.VMEM((4, 128, 512), BF16),
        pltpu.VMEM((2, 4, 4, 256, 128), BF16),
        pltpu.VMEM((2, 3, 4, 256, 128), BF16),
        pltpu.VMEM((2, 4, 256, 128), BF16),
        pltpu.VMEM((2, 3, 256, 128), BF16),
        pltpu.VMEM((128, 512), F32),
        pltpu.VMEM((2, 128, 512), BF16),
        pltpu.VMEM((8, 512, 512), BF16),
        pltpu.VMEM((8, 512, 512), BF16),
        pltpu.VMEM((128, 512), BF16),
        pltpu.VMEM((1024, 512), BF16),
        pltpu.VMEM((1024, 512), F32),
        pltpu.VMEM((8, 128, 512), F32),
        pltpu.VMEM((512, 1024), BF16),
        pltpu.VMEM((8, 128, 512), BF16),
        pltpu.VMEM((2, 128, 256), BF16),
        pltpu.VMEM((2, 128, 512), BF16),
        pltpu.VMEM((8, 128, 256), BF16),
        pltpu.VMEM((16, 32, 512), BF16),
        pltpu.VMEM((16, 32, 512), BF16),
        pltpu.VMEM((16, 32, 512), BF16),
        pltpu.VMEM((16, 32, 512), BF16),
        dma((32,)), dma((64,)),
        dma((14,)), dma((16,)),
        dma((2,)),
        dma((8,)), dma((8,)),
        dma((16,)), dma((16,)),
        dma((4,)), dma((4,)), dma((4,)), dma((4,)),
        dma((6,)), dma((6,)), dma((6,)), dma((6,)),
        dma((2,)),
        dma((2,)), dma((2,)), dma((4,)), dma((8,)),
        dma((8,)), dma((8,)),
        dma((16,)), dma((16,)), dma((16,)), dma((16,)),
    ]
    return pl.pallas_call(
        kernel,
        out_shape=(
            jax.ShapeDtypeStruct((256, 512), BF16),
            jax.ShapeDtypeStruct((1024, 256), BF16),
            jax.ShapeDtypeStruct((1, 32, 512), F32),
            jax.ShapeDtypeStruct((1, 32, 512), F32),
        ),
        in_specs=[pl.BlockSpec(memory_space=pltpu.SMEM)] + [vmem] * 5,
        out_specs=(vmem,) * 4,
        scratch_shapes=scratch,
        compiler_params=pltpu.CompilerParams(
            collective_id=0, has_side_effects=True, vmem_limit_bytes=62 * 1024 * 1024
        ),
    )(logit_scale, text_feats, image_feats, layer_inputs, w_in, w_out)


def solution(mesh):
    placed = (
        P("dp", None),
        P(("dp", "mp"), None),
        P(),
        P("section", "dp", None),
        P("section", None, "mp"),
        P("section", "mp", None),
    )
    return jax.shard_map(
        body,
        mesh=mesh,
        in_specs=placed,
        out_specs=(
            P(("dp", "mp"), None),
            P("dp", "section"),
            P("section", "dp", "mp"),
            P("section", "dp", "mp"),
        ),
        check_vma=False,
    )
```

```python
import functools

import jax
import jax.numpy as jnp
from jax import lax
from jax.experimental import pallas as pl
from jax.experimental.pallas import tpu as pltpu
from jax.sharding import PartitionSpec as P

MESH = pl.DeviceIdType.MESH
F32 = jnp.float32
BF16 = jnp.bfloat16
LOW = -1e30
LOG2E = 1.4426950408889634
PIECES = (
    ((0, 1, 0, 128), (0, 3, 0, 128), (1, 0, 0, 64), (3, 0, 64, 64)),
    ((1, 0, 0, 128), (3, 0, 0, 128), (0, 1, 0, 64), (0, 3, 64, 64)),
)
ORDER = (
    (0, 0), (0, 1), (0, 3), (1, 0), (3, 0), (1, 1), (1, 3), (3, 1),
    (3, 3), (0, 2), (2, 0), (1, 2), (3, 2), (2, 1), (2, 3), (2, 2),
)


def dot_nt(a, b):
    return lax.dot_general(a, b, (((1,), (1,)), ((), ())), preferred_element_type=F32)


def dot_nn(a, b):
    return lax.dot_general(a, b, (((1,), (0,)), ((), ())), preferred_element_type=F32)


def dot_tn(a, b):
    return lax.dot_general(a, b, (((0,), (0,)), ((), ())), preferred_element_type=F32)


def unit_rows(values):
    wide = values.astype(F32)
    length = jnp.sqrt(jnp.sum(wide * wide, axis=1, keepdims=True) + 1.0)
    return wide / length, length


def unit_backward(unit, length, grad):
    return (grad - unit * jnp.sum(unit * grad, axis=1, keepdims=True)) / length


def slope_of(pre):
    s = jax.nn.sigmoid(1.702 * pre)
    return s + 1.702 * pre * s * (1.0 - s)


def rows(start, size=128):
    return pl.ds(pl.multiple_of(start, 128), size)


def copy_to(src, dst, send, recv, device):
    return pltpu.make_async_remote_copy(
        src_ref=src, dst_ref=dst, send_sem=send, recv_sem=recv, device_id=device, device_id_type=MESH
    )


def loop(count, fn, start=0):
    def step(i, _):
        fn(i)
        return 0

    lax.fori_loop(start, count, step, 0)


def kernel(
    scale, text_hbm, image_hbm, hin_hbm, win_hbm, wout_hbm,
    image_out, input_out, first_out, second_out,
    text, image, hin,
    cols, tlow, tlow_t, scores, grads, row_m, row_s, row_a,
    rst, rst_in, rst_a, own_stat, cst, cst_in, col_b,
    tshare, tpass, tshare_in, ishare, relay_in, joined, ifar_in, isum, inear_in, ifull, ihalf,
    wi_all, wo_all, hother, act, slope, slope_own, hin_t, gbuf, gin, gown, inbuf,
    wg, wfar_in, wsum, wnear_in,
    load_s, cols_ss, cols_rs, wx_ss, wx_rs, wy_ss, wy_rs, wd_ss, wd_rs, h_s, rst_ss, rst_rs, cst_ss, cst_rs,
    tp_ss, tp_rs, ts_ss, ts_rs, if_ss, if_rs, ir_ss, ir_rs, ih_s,
    g1_ss, g0_ss, gp_ss, g_rs, in_ss, in_rs,
    wf_ss, wf_rs, wn_ss, wn_rs,
):
    section = lax.axis_index("section")
    dp = lax.axis_index("dp")
    mp = lax.axis_index("mp")
    me = section * 4 + mp
    x, core = me // 2, me % 2
    z, y = dp // 4, dp % 4
    mult = scale[0]
    mult2 = mult * LOG2E

    def line(q):
        return {"section": q // 4, "mp": q % 4}

    def plane(dz, dy):
        return ((z + dz) % 4) * 4 + (y + dy) % 4

    def slot(dz, dy):
        return ORDER.index((dz % 4, dy % 4))

    def away(k):
        return plane(k // 4, k % 4)

    sends = []

    loads = [
        pltpu.make_async_copy(src, dst, load_s.at[n])
        for n, (src, dst) in enumerate(
            (
                (image_hbm.at[rows(section * 128)], image),
                (text_hbm, text),
                (win_hbm.at[0], wi_all.at[0, core]),
                (wout_hbm.at[0], wo_all.at[0, core]),
                (hin_hbm.at[0], hin),
            )
        )
    ]
    for load in loads:
        load.start()

    barrier = pltpu.get_barrier_semaphore()

    def greet_plane(k):
        pl.semaphore_signal(barrier, inc=1, device_id={"dp": away(k)}, device_id_type=MESH)

    def greet_line(i):
        pl.semaphore_signal(barrier, inc=1, device_id=line((me + i) % 8), device_id_type=MESH)

    loop(16, greet_plane, 1)
    loop(8, greet_line, 1)

    loads[0].wait()
    image_unit, image_len = unit_rows(image[...])
    cols[0] = image_unit.astype(BF16)

    def text_block(r):
        unit, _ = unit_rows(text[rows(r * 128), :])
        low = unit.astype(BF16)
        tlow[rows(r * 128), :] = low
        tlow_t[:, rows(r * 128)] = low.astype(F32).T.astype(BF16)
        row_m[rows(r * 128), :] = jnp.full((128, 128), LOW, F32)
        row_s[rows(r * 128), :] = jnp.zeros((128, 128), F32)

    pl.semaphore_wait(barrier, 22)

    def ag_send(dz, dy, lo, size, ez, ey):
        there = slot(dz - ez, dy - ey)
        copy = copy_to(
            cols.at[slot(dz, dy), lo : lo + size],
            cols.at[there, lo : lo + size],
            cols_ss.at[len(sends)],
            cols_rs.at[there * 4 + lo // 32],
            {"dp": plane(ez, ey)},
        )
        copy.start()
        sends.append(copy)

    def ag_wait(dz, dy, lo, size):
        here = slot(dz, dy)
        block = cols.at[here, lo : lo + size]
        copy_to(block, block, cols_ss.at[0], cols_rs.at[here * 4 + lo // 32], {"dp": dp}).wait_recv()

    def flip(swap, *pair):
        return pair[::-1] if swap else pair

    def half_send(swap, first, second, to_first, to_second, lo=0, size=64):
        dz, dy = flip(swap, first, second)
        ez, ey = flip(swap, to_first, to_second)
        ag_send(dz, dy, lo + 64 * swap, size, ez, ey)

    def half_wait(swap, first, second, lo=0, size=64):
        dz, dy = flip(swap, first, second)
        ag_wait(dz, dy, lo + 64 * swap, size)

    for to in ((0, 1), (0, 3), (1, 0), (3, 0)):
        for swap in (0, 1):
            half_send(swap, 0, 0, *to)

    right, left, opposite = (x + 1) % 4, (x + 3) % 4, (x + 2) % 4
    weights = (wi_all, wo_all)

    def weight_rows(which, dz=0, dy=0, lo=0, size=128):
        color = (y + dy + 2 * (z + dz)) % 4 if which == 0 else (2 * (y + dy) + z + dz) % 4
        return pl.ds(pl.multiple_of(color * 128 + lo, 64), size)

    def wx(n, which, src, dst, chip):
        at = weight_rows(which)
        ref = weights[which]
        return copy_to(
            ref.at[src, core, at], ref.at[dst, core, at], wx_ss.at[n], wx_rs.at[which * 4 + dst], line(chip * 2 + core)
        )

    wx_plan = ((0, 0, 3, right), (1, 0, 1, left), (1, 0, 3, right), (0, 0, 1, left), (0, 3, 2, right), (1, 1, 2, left))

    def wx_wait(which, rel):
        block = weights[which].at[rel, core, weight_rows(which)]
        copy_to(block, block, wx_ss.at[0], wx_rs.at[which * 4 + rel], line(me)).wait_recv()

    def wy(which, j):
        dz, dy, lo, size = PIECES[which][j]
        block = weights[which].at[pl.ds(1, 3), core, weight_rows(which, 0, 0, lo, size)]
        n = which * 4 + j
        return copy_to(block, block, wy_ss.at[n], wy_rs.at[n], {"dp": plane(4 - dz, 4 - dy)})

    def wy_wait(which, j):
        block = weights[which].at[pl.ds(1, 3), core, weight_rows(which, *PIECES[which][j])]
        n = which * 4 + j
        copy_to(block, block, wy_ss.at[n], wy_rs.at[n], {"dp": dp}).wait_recv()

    def wd(which, j, side):
        if j < 0:
            block = weights[which].at[0, side]
        else:
            at = weight_rows(which) if j == 4 else weight_rows(which, *PIECES[which][j])
            block = weights[which].at[pl.ds(1, 3), side, at]
        n = which * 6 + j + 1
        return copy_to(block, block, wd_ss.at[n], wd_rs.at[n], line(x * 2 + 1 - core))

    twin = (1 - section) * 4 + mp
    h_copy = copy_to(hin.at[rows(twin * 128), :], hother, h_s.at[0], h_s.at[1], line(twin))
    for load in loads[2:]:
        load.wait()
    for n in range(4):
        wx(n, *wx_plan[n]).start()
    for which in (0, 1):
        wd(which, -1, core).start()
    h_copy.start()

    def score_pair(p):
        pair = cols[pl.ds(2 * p, 2)].reshape(256, 512)
        part = dot_nt(tlow[...], pair)
        c_m, c_s = jnp.full((8, 256), LOW, F32), jnp.zeros((8, 256), F32)
        for r in range(8):
            at = slice(r * 128, (r + 1) * 128)
            s = part[at] * mult2
            scores[p, at, :] = s
            s3 = s.reshape(16, 8, 256)
            n_m = jnp.maximum(c_m, jnp.max(s3, axis=0))
            c_s = c_s * jnp.exp2(c_m - n_m) + jnp.sum(jnp.exp2(s3 - n_m[None]), axis=0)
            c_m = n_m
            old = row_m[at, :]
            s0, s1 = s[:, :128], s[:, 128:]
            new = jnp.maximum(old, jnp.maximum(s0, s1))
            row_s[at, :] = row_s[at, :] * jnp.exp2(old - new) + jnp.exp2(s0 - new) + jnp.exp2(s1 - new)
            row_m[at, :] = new

        peak = jnp.max(c_m, axis=0, keepdims=True)
        total = peak + jnp.log2(jnp.sum(c_s * jnp.exp2(c_m - peak), axis=0, keepdims=True))
        for j in (0, 1):
            own_stat[pl.ds(2 * p + j, 1), :] = total[:, j * 128 : (j + 1) * 128]

    def spread(swap, first, second):
        for to in (1, 3):
            half_send(swap, first, second, to, 0)

    both = (0, 1)
    loads[1].wait()
    loop(8, text_block)
    for swap in both:
        half_wait(swap, 0, 1)
        half_wait(swap, 0, 3)
        half_send(swap, 0, 1, 0, 3, 0, 32)
        half_send(swap, 0, 3, 0, 1, 32, 32)
    for swap in both:
        spread(swap, 0, 1)
        spread(swap, 0, 3)
    for swap in both:
        half_wait(swap, 1, 0)
        half_send(swap, 1, 0, 3, 0)
        half_wait(swap, 3, 0)
    loop(2, score_pair)
    for swap in both:
        half_wait(swap, 0, 2, 0, 32)
        half_wait(swap, 0, 2, 32, 32)
        spread(swap, 0, 2)
    for swap in both:
        for second in (1, 3):
            half_wait(swap, 3, second)
            half_send(swap, 3, second, 1, 0)
            half_wait(swap, 1, second)
    wx_wait(0, 3)
    wx(4, *wx_plan[4]).start()
    wx_wait(1, 1)
    wx(5, *wx_plan[5]).start()
    loop(4, score_pair, 2)
    for swap in both:
        half_wait(swap, 1, 2)
        half_send(swap, 1, 2, 3, 0)
        half_wait(swap, 3, 2)
    for swap in both:
        half_wait(swap, 2, 0)
    half_wait(1, 2, 1)
    loop(6, score_pair, 4)
    half_wait(0, 2, 1)
    for swap in both:
        half_wait(swap, 2, 3)
    for which in both:
        wx_wait(which, 1 if which == 0 else 3)
        wx_wait(which, 2)
    for j in (2, 3):
        for which in both:
            wy(which, j).start()
    for which in both:
        wd(which, 4, core).start()
    loop(7, score_pair, 6)
    for swap in both:
        half_wait(swap, 2, 2)
    score_pair(7)
    for k, (dz, dy) in enumerate(ORDER):
        cst[pl.ds(plane(dz, dy), 1), :] = own_stat[k : k + 1, :]

    def cst_copy(k):
        dz, dy = ORDER[k]
        return copy_to(cst, cst_in.at[dp], cst_ss.at[k], cst_rs.at[dp], {"dp": plane(dz, dy)})

    def cst_wait(k):
        copy_to(cst, cst_in.at[away(k)], cst_ss.at[k], cst_rs.at[away(k)], {"dp": dp}).wait_recv()

    for k in range(15, 0, -1):
        cst_copy(k).start()
    for j in both:
        for which in both:
            wy(which, j).start()
    cst_in[dp] = cst[...]

    for r in range(8):
        m_t = row_m[r * 128 : (r + 1) * 128, :].T
        s_t = row_s[r * 128 : (r + 1) * 128, :].T
        peak = jnp.max(m_t, axis=0, keepdims=True)
        rst[r : r + 1, :] = peak + jnp.log2(jnp.sum(s_t * jnp.exp2(m_t - peak), axis=0, keepdims=True))

    def rst_copy(i):
        q = (me + i) % 8
        return copy_to(rst, rst_in.at[me], rst_ss.at[i], rst_rs.at[me], line(q))

    def rst_wait(i):
        q = (me + i) % 8
        copy_to(rst, rst_in.at[q], rst_ss.at[i], rst_rs.at[q], line(me)).wait_recv()

    loop(8, lambda i: rst_copy(i).start(), 1)
    rst_in[me] = rst[...]

    def hidden_block(r):
        at = rows(r * 128)
        h = hin[at, :]
        pre = dot_nn(h, wi_all[0, core])
        sig = jax.nn.sigmoid(1.702 * pre)
        act[at, :] = (pre * sig).astype(BF16)
        slope[at, :] = sig + 1.702 * pre * sig * (1.0 - sig)
        hin_t[:, at] = h.astype(F32).T.astype(BF16)

    loop(8, hidden_block)

    loop(8, rst_wait, 1)
    peak = jnp.max(rst_in[...], axis=0)
    total = jnp.sum(jnp.exp2(rst_in[...] - peak[None]), axis=0)
    rst_a[...] = peak + jnp.log2(2.0 * total)
    for r in range(8):
        row_a[r * 128 : (r + 1) * 128, :] = jnp.broadcast_to(rst_a[r : r + 1, :], (128, 128)).T

    loop(16, cst_wait, 1)
    peak = jnp.max(cst_in[...], axis=0)
    total = jnp.sum(jnp.exp2(cst_in[...] - peak[None]), axis=0)
    own_stat[...] = peak + jnp.log2(2.0 * total)
    for k, (dz, dy) in enumerate(ORDER):
        col_b[k : k + 1, :] = own_stat[pl.ds(plane(dz, dy), 1), :]

    def prob(s, at, b):
        return jnp.exp2(s - row_a[at, :]) + jnp.exp2(s - b)

    def pass_copy(chip):
        other = chip * 2 + 1 - core
        return copy_to(tshare.at[other], tpass.at[chip], tp_ss.at[chip], tp_rs.at[chip], line(x * 2 + 1 - core))

    def tshare_copy(chip):
        own = chip * 2 + core
        return copy_to(tshare.at[own], tshare_in.at[x], ts_ss.at[chip], ts_rs.at[x], line(own))

    def text_part(chip):
        def grad_block(t):
            p = t % 8
            at = rows(chip * 256 + (t // 8) * 128)
            for j in (0, 1):
                s = scores[p, at, j * 128 : (j + 1) * 128]
                b = col_b[pl.ds(2 * p + j, 1), :]
                grads[at, pl.ds(pl.multiple_of(p * 256 + j * 128, 128), 128)] = prob(s, at, b).astype(BF16)

        loop(16, grad_block)

        mine = 2 * mp + section

        @pl.when(mine // 2 == chip)
        def _():
            at = rows(mine * 128)
            s = scores[0, at, :128]
            eye = lax.broadcasted_iota(jnp.int32, (128, 128), 0) == lax.broadcasted_iota(jnp.int32, (128, 128), 1)
            part = prob(s, at, col_b[0:1, :])
            grads[at, :128] = (part - jnp.where(eye, 1.0, 0.0)).astype(BF16)

        part = dot_nn(grads[rows(chip * 256, 256), :], cols[...].reshape(2048, 512))
        for j in (0, 1):
            tshare[chip * 2 + j] = part[j * 128 : (j + 1) * 128].astype(BF16)
        pass_copy(chip).start()

    def text_merge(chip):
        own = chip * 2 + core
        pass_copy(chip).wait_recv()
        tshare[own] = (tshare[own].astype(F32) + tpass[chip].astype(F32)).astype(BF16)

    def text_step(i):
        chip = jnp.where(i == 0, opposite, jnp.where(i == 1, right, jnp.where(i == 2, left, x)))
        last = jnp.where(i == 1, opposite, jnp.where(i == 2, right, left))
        text_part(chip)

        @pl.when(i > 0)
        def _():
            text_merge(last)
            tshare_copy(last).start()

    def wd_pass(pieces):
        for j in pieces:
            for which in both:
                wy_wait(which, j)
                wd(which, j, core).start()

    wd_pass((2, 3))
    loop(4, text_step)
    text_merge(x)
    wd_pass((0, 1))

    def image_part(p):
        part = dot_nn(tlow_t[...], grads[:, p * 256 : (p + 1) * 256])
        for j in (0, 1):
            dz, dy = ORDER[2 * p + j]
            block = part[:, j * 128 : (j + 1) * 128].astype(BF16)
            ishare[0, dz, dy] = block[:256]
            ishare[1, dy, dz] = block[256:]

    def step_of(swap, far):
        return {"dp": plane(*flip(swap, far, 0))}

    def image_far(n, swap):
        src, dst, to = (
            (ishare.at[swap, 2, 0:2], relay_in.at[swap, 0], 1),
            (ishare.at[swap, 2, 2:4], relay_in.at[swap, 1], 3),
            (ishare.at[swap, 1, 2:4], ifar_in.at[swap, 0, 2:4], 1),
            (ishare.at[swap, 3, 0:2], ifar_in.at[swap, 1, 0:2], 3),
            (joined.at[swap, 0], ifar_in.at[swap, 0, 0:2], 1),
            (joined.at[swap, 1], ifar_in.at[swap, 1, 2:4], 3),
        )[n]
        k = swap * 6 + n
        return copy_to(src, dst, if_ss.at[k], if_rs.at[k], step_of(swap, to))

    def image_near(swap, far):
        n = swap * 3 + 3 - far
        return copy_to(isum.at[swap, far], inear_in.at[swap, 3 - far], ir_ss.at[n], ir_rs.at[n], step_of(1 - swap, far))

    for p in range(7, -1, -1):
        image_part(p)
    for n in range(4):
        for swap in both:
            image_far(n, swap).start()

    def image_relay():
        for n, far, lo in ((0, 1, 0), (1, 3, 2)):
            for swap in both:
                image_far(n, swap).wait_recv()
                joined[swap, n] = (
                    ishare[swap, far, lo : lo + 2].astype(F32) + relay_in[swap, n].astype(F32)
                ).astype(BF16)
                image_far(n + 4, swap).start()


    h_copy.wait_recv()

    for j in range(-1, 5):
        for which in both:
            wd(which, j, 1 - core).wait_recv()

    def home(q):
        return (q // 2 + 4 - x) % 4, q % 2

    def own_block(r):
        h = jnp.where(r // 4 == section, hin[rows(me * 128), :], hother[...])
        slope_own[r] = slope_of(dot_nn(h, wi_all[home(r)]))

    loop(8, own_block)

    def tshare_sum(i, acc):
        chip = (x + i) % 4
        copy_to(tshare.at[0], tshare_in.at[chip], ts_ss.at[chip], ts_rs.at[chip], line(me)).wait_recv()
        return acc + tshare_in[chip].astype(F32)

    total = lax.fori_loop(1, 4, tshare_sum, tshare[me].astype(F32)) * mult
    unit, length = unit_rows(text[rows(me * 128), :])
    gown[0] = unit_backward(unit, length, total).astype(BF16)

    def g_copy(layer, lo, sems):
        to = {"section": layer, "mp": lo * 2 + core}
        return copy_to(gown.at[1 - layer], gbuf.at[me], sems.at[lo], g_rs.at[me], to)

    def g_send(layer, sems):
        for lo in (0, 1):
            pl.when(x != layer * 2 + lo)(lambda lo=lo: g_copy(layer, lo, sems).start())

        @pl.when(section == layer)
        def _():
            gbuf[me] = gown[1 - layer]

    def g_pass(i):
        q = ((x + i) % 4) * 2 + core
        return copy_to(gbuf.at[q], gbuf.at[q], gp_ss.at[i], g_rs.at[q], line(x * 2 + 1 - core))

    def g_arrive(q):
        copy_to(gbuf.at[q], gbuf.at[q], gp_ss.at[0], g_rs.at[q], line(me)).wait_recv()

    def g_relay(i):
        g_arrive(((x + i) % 4) * 2 + core)
        g_pass(i).start()

    def chain(layer):
        g = gown[1 - layer]

        def step(j, acc):
            q = layer * 4 + j
            back = dot_nt(g, wo_all[home(q)])
            pre_grad = (back * slope_own[q]).astype(BF16)
            return acc + dot_nt(pre_grad, wi_all[home(q)])

        return lax.fori_loop(0, 4, step, g.astype(F32)).astype(BF16)

    g_send(1, g1_ss)
    gown[1] = chain(1)
    g_send(0, g0_ss)
    image_relay()
    lowest = chain(0)
    gin[0] = lowest[:, :256]
    gin[1] = lowest[:, 256:]

    def in_copy(i):
        q = (me + i) % 8
        return copy_to(gin.at[q // 4], inbuf.at[me], in_ss.at[i], in_rs.at[me], line(q))

    def image_fold(swap):
        for n in range(2, 6):
            image_far(n, swap).wait_recv()
        total = ishare[swap, 0].astype(F32) + ifar_in[swap, 0].astype(F32) + ifar_in[swap, 1].astype(F32)
        isum[swap] = total.astype(BF16)
        for far in (2, 1, 3):
            image_near(swap, far).start()

    g_pass(0).start()
    loop(4, g_relay, 1)
    loop(8, lambda i: in_copy(i).start(), 1)
    inbuf[me] = gin[section]
    for swap in both:
        image_fold(swap)
    loop(4, lambda i: g_arrive(((x + i) % 4) * 2 + 1 - core))

    full = gbuf[...].reshape(1024, 512)

    def put_weight(which, value):
        for zz in range(4):
            for yy in range(4):
                block = value[(zz * 4 + yy) * 32 : (zz * 4 + yy + 1) * 32].astype(BF16)
                wg[which, 0, zz, yy] = block[:, :256]
                wg[which, 1, yy, zz] = block[:, 256:]

    def weight_far(which, swap, far):
        n = which * 6 + swap * 3 + 3 - far
        at = ((y if swap else z) + far) % 4
        return copy_to(
            wg.at[which, swap, at], wfar_in.at[which, swap, 3 - far], wf_ss.at[n], wf_rs.at[n], step_of(swap, far)
        )

    def weight_near(which, swap, far):
        n = which * 6 + swap * 3 + 3 - far
        at = ((z if swap else y) + far) % 4
        return copy_to(
            wsum.at[which, swap, at], wnear_in.at[which, swap, 3 - far], wn_ss.at[n], wn_rs.at[n], step_of(1 - swap, far)
        )

    def send_all(step, which):
        for far in (2, 1, 3):
            for swap in both:
                step(which, swap, far).start()

    def weight_fold(which):
        for swap in both:
            total = wg[which, swap, y if swap else z].astype(F32)
            for far in (1, 2, 3):
                landed = wfar_in.at[which, swap, far - 1]
                n = which * 6 + swap * 3 + far - 1
                copy_to(landed, landed, wf_ss.at[n], wf_rs.at[n], {"dp": dp}).wait_recv()
                total = total + landed[...].astype(F32)
            wsum[which, swap] = total.astype(BF16)
        send_all(weight_near, which)

    def weight_end(which, out):
        for swap in both:
            total = wsum[which, swap, z if swap else y].astype(F32)
            for far in (1, 2, 3):
                landed = wnear_in.at[which, swap, far - 1]
                n = which * 6 + swap * 3 + far - 1
                copy_to(landed, landed, wn_ss.at[n], wn_rs.at[n], {"dp": dp}).wait_recv()
                total = total + landed[...].astype(F32)
            out[0, :, swap * 256 : (swap + 1) * 256] = total

    put_weight(1, dot_tn(full, act[...]))
    send_all(weight_far, 1)

    def back_block(r):
        at = rows(r * 256, 256)
        back = dot_nt(gbuf[pl.ds(2 * r, 2)].reshape(256, 512), wo_all[0, core])
        act[at, :] = (back * slope[at, :]).astype(BF16)

    loop(4, back_block)
    put_weight(0, dot_nn(hin_t[...], act[...]))
    send_all(weight_far, 0)

    for swap in both:
        total = isum[swap, 0].astype(F32)
        for far in (1, 2, 3):
            landed = inear_in.at[swap, far - 1]
            copy_to(landed, landed, ir_ss.at[0], ir_rs.at[swap * 3 + far - 1], {"dp": dp}).wait_recv()
            total = total + landed[...].astype(F32)
        ifull[:, swap * 256 : (swap + 1) * 256] = total.T
    total = ifull[...] * mult
    image_unit, image_len = unit_rows(image[...])
    ihalf[0] = unit_backward(image_unit, image_len, total).astype(BF16)
    ihalf_copy = copy_to(ihalf.at[0], ihalf.at[1], ih_s.at[0], ih_s.at[1], line(twin))
    ihalf_copy.start()
    weight_fold(1)

    def in_wait(i):
        q = (me + i) % 8
        copy_to(gin.at[0], inbuf.at[q], in_ss.at[i], in_rs.at[q], line(me)).wait_recv()

    loop(8, in_wait, 1)
    input_out[...] = inbuf[...].reshape(1024, 256)

    weight_fold(0)
    image_out[rows(section * 128), :] = ihalf[0]
    ihalf_copy.wait_recv()
    image_out[rows((1 - section) * 128), :] = ihalf[1]
    weight_end(1, second_out)
    weight_end(0, first_out)
    for copy in sends:
        copy.wait_send()
    h_copy.wait_send()
    for n in range(6):
        wx(n, *wx_plan[n]).wait_send()
    for which in both:
        for j in range(4):
            wy(which, j).wait_send()
        for j in range(-1, 5):
            wd(which, j, core).wait_send()
    for k in range(1, 16):
        cst_copy(k).wait_send()
    loop(8, lambda i: rst_copy(i).wait_send(), 1)
    loop(4, lambda i: pass_copy(i).wait_send())
    loop(4, lambda i: tshare_copy((x + i) % 4).wait_send(), 1)
    for swap in both:
        for far in (1, 2, 3):
            image_near(swap, far).wait_send()
        for n in range(6):
            image_far(n, swap).wait_send()
    ihalf_copy.wait_send()
    for layer, sems in ((1, g1_ss), (0, g0_ss)):
        for lo in (0, 1):
            pl.when(x != layer * 2 + lo)(lambda lo=lo, layer=layer, sems=sems: g_copy(layer, lo, sems).wait_send())
    loop(4, lambda i: g_pass(i).wait_send())
    loop(8, lambda i: in_copy(i).wait_send(), 1)
    for which in both:
        for swap in both:
            for far in (1, 2, 3):
                weight_far(which, swap, far).wait_send()
                weight_near(which, swap, far).wait_send()


def settle(*refs):
    for src, dst in zip(refs[:4], refs[4:]):
        dst[...] = src[...]


def body(text_feats, image_feats, logit_scale, layer_inputs, w_in, w_out):
    vmem = pl.BlockSpec(memory_space=pltpu.VMEM)
    dma = pltpu.SemaphoreType.DMA
    scratch = [
        pltpu.VMEM((1024, 512), BF16),
        pltpu.VMEM((128, 512), BF16),
        pltpu.VMEM((1024, 512), BF16),
        pltpu.VMEM((16, 128, 512), BF16),
        pltpu.VMEM((1024, 512), BF16),
        pltpu.VMEM((512, 1024), BF16),
        pltpu.VMEM((8, 1024, 256), F32),
        pltpu.VMEM((1024, 2048), BF16),
        pltpu.VMEM((1024, 128), F32),
        pltpu.VMEM((1024, 128), F32),
        pltpu.VMEM((1024, 128), F32),
        pltpu.VMEM((8, 128), F32),
        pltpu.VMEM((8, 8, 128), F32),
        pltpu.VMEM((8, 128), F32),
        pltpu.VMEM((16, 128), F32),
        pltpu.VMEM((16, 128), F32),
        pltpu.VMEM((16, 16, 128), F32),
        pltpu.VMEM((16, 128), F32),
        pltpu.VMEM((8, 128, 512), BF16),
        pltpu.VMEM((4, 128, 512), BF16),
        pltpu.VMEM((4, 128, 512), BF16),
        pltpu.VMEM((2, 4, 4, 256, 128), BF16),
        pltpu.VMEM((2, 2, 2, 256, 128), BF16),
        pltpu.VMEM((2, 2, 2, 256, 128), BF16),
        pltpu.VMEM((2, 2, 4, 256, 128), BF16),
        pltpu.VMEM((2, 4, 256, 128), BF16),
        pltpu.VMEM((2, 3, 256, 128), BF16),
        pltpu.VMEM((128, 512), F32),
        pltpu.VMEM((2, 128, 512), BF16),
        pltpu.VMEM((4, 2, 512, 512), BF16),
        pltpu.VMEM((4, 2, 512, 512), BF16),
        pltpu.VMEM((128, 512), BF16),
        pltpu.VMEM((1024, 512), BF16),
        pltpu.VMEM((1024, 512), F32),
        pltpu.VMEM((8, 128, 512), F32),
        pltpu.VMEM((512, 1024), BF16),
        pltpu.VMEM((8, 128, 512), BF16),
        pltpu.VMEM((2, 128, 256), BF16),
        pltpu.VMEM((2, 128, 512), BF16),
        pltpu.VMEM((8, 128, 256), BF16),
        pltpu.VMEM((2, 2, 4, 4, 32, 256), BF16),
        pltpu.VMEM((2, 2, 3, 4, 32, 256), BF16),
        pltpu.VMEM((2, 2, 4, 32, 256), BF16),
        pltpu.VMEM((2, 2, 3, 32, 256), BF16),
        dma((5,)),
        dma((32,)), dma((64,)),
        dma((6,)), dma((8,)), dma((8,)), dma((8,)), dma((12,)), dma((12,)),
        dma((2,)),
        dma((8,)), dma((8,)),
        dma((16,)), dma((16,)),
        dma((4,)), dma((4,)), dma((4,)), dma((4,)),
        dma((12,)), dma((12,)), dma((6,)), dma((6,)),
        dma((2,)),
        dma((2,)), dma((2,)), dma((4,)), dma((8,)),
        dma((8,)), dma((8,)),
        dma((12,)), dma((12,)), dma((12,)), dma((12,)),
    ]
    results = pl.pallas_call(
        kernel,
        out_shape=(
            jax.ShapeDtypeStruct((256, 512), BF16),
            jax.ShapeDtypeStruct((1024, 256), BF16),
            jax.ShapeDtypeStruct((1, 32, 512), F32),
            jax.ShapeDtypeStruct((1, 32, 512), F32),
        ),
        in_specs=[pl.BlockSpec(memory_space=pltpu.SMEM)] + [pl.BlockSpec(memory_space=pl.ANY)] * 5,
        out_specs=(vmem,) * 4,
        scratch_shapes=scratch,
        compiler_params=pltpu.CompilerParams(
            collective_id=0, has_side_effects=True, vmem_limit_bytes=56 * 1024 * 1024
        ),
    )(logit_scale, text_feats, image_feats, layer_inputs, w_in, w_out)
    return pl.pallas_call(
        settle,
        out_shape=tuple(jax.ShapeDtypeStruct(r.shape, r.dtype) for r in results),
        in_specs=[vmem] * 4,
        out_specs=(vmem,) * 4,
    )(*results)


def solution(mesh):
    placed = (
        P("dp", None),
        P(("dp", "mp"), None),
        P(),
        P("section", "dp", None),
        P("section", None, "mp"),
        P("section", "mp", None),
    )
    return jax.shard_map(
        body,
        mesh=mesh,
        in_specs=placed,
        out_specs=(
            P(("dp", "mp"), None),
            P("dp", "section"),
            P("section", "dp", "mp"),
            P("section", "dp", "mp"),
        ),
        check_vma=False,
    )
```

```python
import functools

import jax
import jax.numpy as jnp
from jax import lax
from jax.experimental import pallas as pl
from jax.experimental.pallas import tpu as pltpu
from jax.sharding import PartitionSpec as P

MESH = pl.DeviceIdType.MESH
F32 = jnp.float32
BF16 = jnp.bfloat16
LOW = -1e30
LOG2E = 1.4426950408889634
AROUND = ((0, 1), (0, 3), (1, 0), (3, 0))
ORDER = (
    (0, 0), (0, 1), (0, 3), (1, 0), (3, 0), (1, 1), (1, 3), (3, 1),
    (3, 3), (0, 2), (2, 0), (1, 2), (3, 2), (2, 1), (2, 3), (2, 2),
)


def dot_nt(a, b):
    return lax.dot_general(a, b, (((1,), (1,)), ((), ())), preferred_element_type=F32)


def dot_nn(a, b):
    return lax.dot_general(a, b, (((1,), (0,)), ((), ())), preferred_element_type=F32)


def dot_tn(a, b):
    return lax.dot_general(a, b, (((0,), (0,)), ((), ())), preferred_element_type=F32)


def unit_rows(values):
    wide = values.astype(F32)
    length = jnp.sqrt(jnp.sum(wide * wide, axis=1, keepdims=True) + 1.0)
    return wide / length, length


def unit_backward(unit, length, grad):
    return (grad - unit * jnp.sum(unit * grad, axis=1, keepdims=True)) / length


def slope_of(pre):
    s = jax.nn.sigmoid(1.702 * pre)
    return s + 1.702 * pre * s * (1.0 - s)


def rows(start, size=128):
    return pl.ds(pl.multiple_of(start, 128), size)


def copy_to(src, dst, send, recv, device):
    return pltpu.make_async_remote_copy(
        src_ref=src, dst_ref=dst, send_sem=send, recv_sem=recv, device_id=device, device_id_type=MESH
    )


def loop(count, fn, start=0):
    def step(i, _):
        fn(i)
        return 0

    lax.fori_loop(start, count, step, 0)


def kernel(
    scale, text_hbm, image_hbm, hin_hbm, win_hbm, wout_hbm,
    image_out, input_out, first_out, second_out,
    text, image, hin,
    cols, tlow, tlow_t, scores, grads0, grads1, grads2, grads3, row_m, row_s, row_a,
    rst, rst_in, rst_a, own_stat, cst, cst_in, col_b,
    tshare, tpass, tshare_in, ishare, relay_in, joined, ifar_in, isum, inear_in, ifull, ihalf,
    wi_all, wo_all, hother, act, slope, slope_own, hin_t, gbuf, gin, gown, inbuf,
    wacc, wg, wrelay_in, wjoined, wfar_in, wsum, wnear_in,
    load_s, cols_ss, cols_rs, wx_ss, wx_rs, wy_ss, wy_rs, wd_ss, wd_rs, h_s, rst_ss, rst_rs, cst_ss, cst_rs,
    tp_ss, tp_rs, ts_ss, ts_rs, if_ss, if_rs, ir_ss, ir_rs, ih_s,
    g1_ss, g0_ss, gf_ss, g_rs, gp_ss, gp_rs, in_ss, in_rs,
    wf_ss, wf_rs, wn_ss, wn_rs,
):
    section = lax.axis_index("section")
    dp = lax.axis_index("dp")
    mp = lax.axis_index("mp")
    me = section * 4 + mp
    x, core = me // 2, me % 2
    z, y = dp // 4, dp % 4
    mult = scale[0]
    mult2 = mult * LOG2E

    def line(q):
        return {"section": q // 4, "mp": q % 4}

    def plane(dz, dy):
        return ((z + dz) % 4) * 4 + (y + dy) % 4

    def slot(dz, dy):
        return ORDER.index((dz % 4, dy % 4))

    def away(k):
        return plane(k // 4, k % 4)

    sends = []

    loads = [
        pltpu.make_async_copy(src, dst, load_s.at[n])
        for n, (src, dst) in enumerate(
            (
                (image_hbm.at[rows(section * 128)], image),
                (text_hbm, text),
                (win_hbm.at[0], wi_all.at[0, core]),
                (wout_hbm.at[0], wo_all.at[0, core]),
                (hin_hbm.at[0], hin),
            )
        )
    ]
    for load in loads:
        load.start()

    barrier = pltpu.get_barrier_semaphore()

    def greet_plane(k):
        pl.semaphore_signal(barrier, inc=1, device_id={"dp": away(k)}, device_id_type=MESH)

    def greet_line(i):
        pl.semaphore_signal(barrier, inc=1, device_id=line((me + i) % 8), device_id_type=MESH)

    loop(16, greet_plane, 1)
    loop(8, greet_line, 1)

    loads[0].wait()
    image_unit, image_len = unit_rows(image[...])
    cols[0] = image_unit.astype(BF16)

    def text_block(r):
        unit, _ = unit_rows(text[rows(r * 128), :])
        low = unit.astype(BF16)
        tlow[rows(r * 128), :] = low
        tlow_t[:, rows(r * 128)] = low.astype(F32).T.astype(BF16)
        row_m[rows(r * 128), :] = jnp.full((128, 128), LOW, F32)
        row_s[rows(r * 128), :] = jnp.zeros((128, 128), F32)

    pl.semaphore_wait(barrier, 22)

    def ag_send(dz, dy, lo, size, ez, ey):
        there = slot(dz - ez, dy - ey)
        copy = copy_to(
            cols.at[slot(dz, dy), lo : lo + size],
            cols.at[there, lo : lo + size],
            cols_ss.at[len(sends)],
            cols_rs.at[there * 4 + lo // 32],
            {"dp": plane(ez, ey)},
        )
        copy.start()
        sends.append(copy)

    def ag_wait(dz, dy, lo, size):
        here = slot(dz, dy)
        block = cols.at[here, lo : lo + size]
        copy_to(block, block, cols_ss.at[0], cols_rs.at[here * 4 + lo // 32], {"dp": dp}).wait_recv()

    def flip(swap, *pair):
        return pair[::-1] if swap else pair

    def half_send(swap, first, second, to_first, to_second, lo=0, size=64):
        dz, dy = flip(swap, first, second)
        ez, ey = flip(swap, to_first, to_second)
        ag_send(dz, dy, lo + 64 * swap, size, ez, ey)

    def half_wait(swap, first, second, lo=0, size=64):
        dz, dy = flip(swap, first, second)
        ag_wait(dz, dy, lo + 64 * swap, size)

    for to in ((0, 1), (0, 3), (1, 0), (3, 0)):
        for swap in (0, 1):
            half_send(swap, 0, 0, *to)

    right, left, opposite = (x + 1) % 4, (x + 3) % 4, (x + 2) % 4
    weights = (wi_all, wo_all)

    def weight_rows(turn, lo=0, size=256):
        return pl.ds(pl.multiple_of((y + z + turn) % 2 * 256 + lo, 64), size)

    def wx(n, which, src, dst, chip):
        at = weight_rows(0)
        ref = weights[which]
        return copy_to(
            ref.at[src, core, at], ref.at[dst, core, at], wx_ss.at[n], wx_rs.at[which * 4 + dst], line(chip * 2 + core)
        )

    wx_plan = ((0, 0, 3, right), (1, 0, 1, left), (1, 0, 3, right), (0, 0, 1, left), (0, 3, 2, right), (1, 1, 2, left))

    def wx_wait(which, rel):
        block = weights[which].at[rel, core, weight_rows(0)]
        copy_to(block, block, wx_ss.at[0], wx_rs.at[which * 4 + rel], line(me)).wait_recv()

    def wy(which, j):
        dz, dy = AROUND[j]
        block = weights[which].at[pl.ds(1, 3), core, weight_rows(0, j * 64, 64)]
        n = which * 4 + j
        return copy_to(block, block, wy_ss.at[n], wy_rs.at[n], {"dp": plane(4 - dz, 4 - dy)})

    def wy_wait(which, j):
        block = weights[which].at[pl.ds(1, 3), core, weight_rows(1, j * 64, 64)]
        n = which * 4 + j
        copy_to(block, block, wy_ss.at[n], wy_rs.at[n], {"dp": dp}).wait_recv()

    def wd(which, j, side):
        if j < 0:
            block = weights[which].at[0, side]
        else:
            at = weight_rows(0) if j == 4 else weight_rows(1, j * 64, 64)
            block = weights[which].at[pl.ds(1, 3), side, at]
        n = which * 6 + j + 1
        return copy_to(block, block, wd_ss.at[n], wd_rs.at[n], line(x * 2 + 1 - core))

    twin = (1 - section) * 4 + mp
    h_copy = copy_to(hin.at[rows(twin * 128), :], hother, h_s.at[0], h_s.at[1], line(twin))
    for load in loads[2:]:
        load.wait()
    for n in range(4):
        wx(n, *wx_plan[n]).start()
    for which in (0, 1):
        wd(which, -1, core).start()
    h_copy.start()

    def score_pair(p):
        pair = cols[pl.ds(2 * p, 2)].reshape(256, 512)
        part = dot_nt(tlow[...], pair)
        c_m, c_s = jnp.full((8, 256), LOW, F32), jnp.zeros((8, 256), F32)
        for r in range(8):
            at = slice(r * 128, (r + 1) * 128)
            s = part[at] * mult2
            scores[p, at, :] = s
            s3 = s.reshape(16, 8, 256)
            n_m = jnp.maximum(c_m, jnp.max(s3, axis=0))
            c_s = c_s * jnp.exp2(c_m - n_m) + jnp.sum(jnp.exp2(s3 - n_m[None]), axis=0)
            c_m = n_m
            old = row_m[at, :]
            s0, s1 = s[:, :128], s[:, 128:]
            new = jnp.maximum(old, jnp.maximum(s0, s1))
            row_s[at, :] = row_s[at, :] * jnp.exp2(old - new) + jnp.exp2(s0 - new) + jnp.exp2(s1 - new)
            row_m[at, :] = new

        peak = jnp.max(c_m, axis=0, keepdims=True)
        total = peak + jnp.log2(jnp.sum(c_s * jnp.exp2(c_m - peak), axis=0, keepdims=True))
        for j in (0, 1):
            own_stat[pl.ds(2 * p + j, 1), :] = total[:, j * 128 : (j + 1) * 128]

    def spread(swap, first, second):
        for to in (1, 3):
            half_send(swap, first, second, to, 0)

    both = (0, 1)
    loads[1].wait()
    loop(8, text_block)
    for swap in both:
        half_wait(swap, 0, 1)
        half_wait(swap, 0, 3)
        half_send(swap, 0, 1, 0, 3, 0, 32)
        half_send(swap, 0, 3, 0, 1, 32, 32)
    for swap in both:
        spread(swap, 0, 1)
        spread(swap, 0, 3)
    for swap in both:
        half_wait(swap, 1, 0)
        half_send(swap, 1, 0, 3, 0)
        half_wait(swap, 3, 0)
    loop(2, score_pair)
    for swap in both:
        half_wait(swap, 0, 2, 0, 32)
        half_wait(swap, 0, 2, 32, 32)
        spread(swap, 0, 2)
    for swap in both:
        for second in (1, 3):
            half_wait(swap, 3, second)
            half_send(swap, 3, second, 1, 0)
            half_wait(swap, 1, second)
    wx_wait(0, 3)
    wx(4, *wx_plan[4]).start()
    wx_wait(1, 1)
    wx(5, *wx_plan[5]).start()
    loop(4, score_pair, 2)
    for swap in both:
        half_wait(swap, 1, 2)
        half_send(swap, 1, 2, 3, 0)
        half_wait(swap, 3, 2)
    for swap in both:
        half_wait(swap, 2, 0)
    half_wait(1, 2, 1)
    loop(6, score_pair, 4)
    half_wait(0, 2, 1)
    for swap in both:
        half_wait(swap, 2, 3)
    loop(7, score_pair, 6)
    for swap in both:
        half_wait(swap, 2, 2)
    score_pair(7)
    for k, (dz, dy) in enumerate(ORDER):
        cst[pl.ds(plane(dz, dy), 1), :] = own_stat[k : k + 1, :]

    def cst_copy(k):
        dz, dy = ORDER[k]
        return copy_to(cst, cst_in.at[dp], cst_ss.at[k], cst_rs.at[dp], {"dp": plane(dz, dy)})

    def cst_wait(k):
        copy_to(cst, cst_in.at[away(k)], cst_ss.at[k], cst_rs.at[away(k)], {"dp": dp}).wait_recv()

    for k in range(15, 0, -1):
        cst_copy(k).start()
    cst_in[dp] = cst[...]

    for r in range(8):
        m_t = row_m[r * 128 : (r + 1) * 128, :].T
        s_t = row_s[r * 128 : (r + 1) * 128, :].T
        peak = jnp.max(m_t, axis=0, keepdims=True)
        rst[r : r + 1, :] = peak + jnp.log2(jnp.sum(s_t * jnp.exp2(m_t - peak), axis=0, keepdims=True))

    def rst_copy(i):
        q = (me + i) % 8
        return copy_to(rst, rst_in.at[me], rst_ss.at[i], rst_rs.at[me], line(q))

    def rst_wait(i):
        q = (me + i) % 8
        copy_to(rst, rst_in.at[q], rst_ss.at[i], rst_rs.at[q], line(me)).wait_recv()

    loop(8, lambda i: rst_copy(i).start(), 1)
    rst_in[me] = rst[...]

    def hidden_block(r):
        at = rows(r * 128)
        h = hin[at, :]
        pre = dot_nn(h, wi_all[0, core])
        sig = jax.nn.sigmoid(1.702 * pre)
        act[at, :] = (pre * sig).astype(BF16)
        slope[at, :] = sig + 1.702 * pre * sig * (1.0 - sig)
        hin_t[:, at] = h.astype(F32).T.astype(BF16)

    loop(8, hidden_block)

    loop(8, rst_wait, 1)
    peak = jnp.max(rst_in[...], axis=0)
    total = jnp.sum(jnp.exp2(rst_in[...] - peak[None]), axis=0)
    rst_a[...] = peak + jnp.log2(2.0 * total)
    for r in range(8):
        row_a[r * 128 : (r + 1) * 128, :] = jnp.broadcast_to(rst_a[r : r + 1, :], (128, 128)).T

    loop(16, cst_wait, 1)
    peak = jnp.max(cst_in[...], axis=0)
    total = jnp.sum(jnp.exp2(cst_in[...] - peak[None]), axis=0)
    own_stat[...] = peak + jnp.log2(2.0 * total)
    for k, (dz, dy) in enumerate(ORDER):
        col_b[k : k + 1, :] = own_stat[pl.ds(plane(dz, dy), 1), :]

    def pass_copy(chip):
        other = chip * 2 + 1 - core
        return copy_to(tshare.at[other], tpass.at[chip], tp_ss.at[chip], tp_rs.at[chip], line(x * 2 + 1 - core))

    def tshare_copy(chip):
        own = chip * 2 + core
        return copy_to(tshare.at[own], tshare_in.at[x], ts_ss.at[chip], ts_rs.at[x], line(own))

    chips = (opposite, right, left, x)
    parts = (grads0, grads1, grads2, grads3)
    mine = 2 * mp + section
    eye = (
        lax.broadcasted_iota(jnp.int32, (128, 128), 0) == lax.broadcasted_iota(jnp.int32, (128, 128), 1)
    ).astype(F32)

    def make_grads(i):
        for half in both:
            at = rows(chips[i] * 256 + half * 128)
            a = row_a[at, :]
            for k in range(16):
                p, j = k // 2, k % 2
                s = scores[p, at, j * 128 : (j + 1) * 128]
                part = jnp.exp2(s - a) + jnp.exp2(s - col_b[k : k + 1, :])
                if k == 0:
                    part = part - eye * jnp.where(chips[i] * 2 + half == mine, 1.0, 0.0)
                parts[i][half * 128 : (half + 1) * 128, k * 128 : (k + 1) * 128] = part.astype(BF16)

    def text_merge(chip):
        own = chip * 2 + core
        pass_copy(chip).wait_recv()
        tshare[own] = (tshare[own].astype(F32) + tpass[chip].astype(F32)).astype(BF16)

    def wd_pass(which):
        for j in range(4):
            wy_wait(which, j)
            wd(which, j, core).start()

    def wd_wait(which):
        for j in range(-1, 5):
            wd(which, j, 1 - core).wait_recv()

    for which in both:
        wx_wait(which, 1 if which == 0 else 3)
        wx_wait(which, 2)
    for which in both:
        for j in range(4):
            wy(which, j).start()
    for which in both:
        wd(which, 4, core).start()
    make_grads(0)
    for i in range(4):
        if i < 3:
            make_grads(i + 1)
        part = dot_nn(parts[i][...], cols[...].reshape(2048, 512))
        for j in (0, 1):
            tshare[chips[i] * 2 + j] = part[j * 128 : (j + 1) * 128].astype(BF16)
        pass_copy(chips[i]).start()
        if i > 0:
            text_merge(chips[i - 1])
            tshare_copy(chips[i - 1]).start()
    text_merge(x)
    wd_pass(0)

    def image_part(p):
        part = sum(
            dot_nn(tlow_t[:, rows(chips[i] * 256, 256)], parts[i][:, p * 256 : (p + 1) * 256]) for i in range(4)
        )
        for j in (0, 1):
            dz, dy = ORDER[2 * p + j]
            block = part[:, j * 128 : (j + 1) * 128].astype(BF16)
            ishare[0, dz, dy] = block[:256]
            ishare[1, dy, dz] = block[256:]

    def step_of(swap, far):
        return {"dp": plane(*flip(swap, far, 0))}

    def image_far(n, swap):
        src, dst, to = (
            (ishare.at[swap, 2, 0:2], relay_in.at[swap, 0], 1),
            (ishare.at[swap, 2, 2:4], relay_in.at[swap, 1], 3),
            (ishare.at[swap, 1, 2:4], ifar_in.at[swap, 0, 2:4], 1),
            (ishare.at[swap, 3, 0:2], ifar_in.at[swap, 1, 0:2], 3),
            (joined.at[swap, 0], ifar_in.at[swap, 0, 0:2], 1),
            (joined.at[swap, 1], ifar_in.at[swap, 1, 2:4], 3),
        )[n]
        k = swap * 6 + n
        return copy_to(src, dst, if_ss.at[k], if_rs.at[k], step_of(swap, to))

    def image_near(swap, far):
        n = swap * 3 + 3 - far
        return copy_to(isum.at[swap, far], inear_in.at[swap, 3 - far], ir_ss.at[n], ir_rs.at[n], step_of(1 - swap, far))

    for p in range(7, -1, -1):
        image_part(p)
    for n in range(4):
        for swap in both:
            image_far(n, swap).start()

    def image_relay():
        for n, far, lo in ((0, 1, 0), (1, 3, 2)):
            for swap in both:
                image_far(n, swap).wait_recv()
                joined[swap, n] = (
                    ishare[swap, far, lo : lo + 2].astype(F32) + relay_in[swap, n].astype(F32)
                ).astype(BF16)
                image_far(n + 4, swap).start()


    wd_pass(1)
    h_copy.wait_recv()

    wd_wait(0)

    def home(q):
        return (q // 2 + 4 - x) % 4, q % 2

    def own_block(r):
        h = jnp.where(r // 4 == section, hin[rows(me * 128), :], hother[...])
        slope_own[r] = slope_of(dot_nn(h, wi_all[home(r)]))

    loop(8, own_block, 4)

    def tshare_sum(i, acc):
        chip = (x + i) % 4
        copy_to(tshare.at[0], tshare_in.at[chip], ts_ss.at[chip], ts_rs.at[chip], line(me)).wait_recv()
        return acc + tshare_in[chip].astype(F32)

    total = lax.fori_loop(1, 4, tshare_sum, tshare[me].astype(F32)) * mult
    unit, length = unit_rows(text[rows(me * 128), :])
    gown[0] = unit_backward(unit, length, total).astype(BF16)

    sibling = x + 1 - 2 * (x % 2)

    def g_copy(layer, half, sems):
        at = pl.ds(half * 64, 64)
        to = jnp.where(section == layer, sibling, 3 - x) * 2 + core
        return copy_to(gown.at[1 - layer, at], gbuf.at[me, at], sems.at[half], g_rs.at[me * 2 + half], line(to))

    def g_send(layer, sems):
        for half in both:
            g_copy(layer, half, sems).start()

        @pl.when(section == layer)
        def _():
            gbuf[me] = gown[1 - layer]

    def g_forward(half):
        q = (3 - x) * 2 + core
        block = gbuf.at[q, pl.ds(half * 64, 64)]
        return copy_to(block, block, gf_ss.at[half], g_rs.at[q * 2 + half], line(sibling * 2 + core))

    def g_arrive(chip):
        q = chip * 2 + core
        for half in both:
            block = gbuf.at[q, pl.ds(half * 64, 64)]
            copy_to(block, block, gf_ss.at[0], g_rs.at[q * 2 + half], line(me)).wait_recv()

    def order_of(i):
        return jnp.where(i == 0, x, jnp.where(i == 1, sibling, jnp.where(i == 2, 3 - x, 3 - sibling)))

    def g_pass(i):
        chip = order_of(i)
        block = gbuf.at[chip * 2 + core]
        return copy_to(block, block, gp_ss.at[i], gp_rs.at[chip], line(x * 2 + 1 - core))

    def g_passed(chip):
        block = gbuf.at[chip * 2 + 1 - core]
        copy_to(block, block, gp_ss.at[0], gp_rs.at[chip], line(me)).wait_recv()

    def chain(layer):
        g = gown[1 - layer]

        def step(j, acc):
            q = layer * 4 + j
            back = dot_nt(g, wo_all[home(q)])
            pre_grad = (back * slope_own[q]).astype(BF16)
            return acc + dot_nt(pre_grad, wi_all[home(q)])

        return lax.fori_loop(0, 4, step, g.astype(F32)).astype(BF16)

    wd_wait(1)
    g_send(1, g1_ss)
    gown[1] = chain(1)
    g_send(0, g0_ss)
    loop(4, own_block)
    image_relay()
    lowest = chain(0)
    gin[0] = lowest[:, :256]
    gin[1] = lowest[:, 256:]

    def in_copy(i):
        q = (me + i) % 8
        return copy_to(gin.at[q // 4], inbuf.at[me], in_ss.at[i], in_rs.at[me], line(q))

    def image_fold(swap):
        for n in range(2, 6):
            image_far(n, swap).wait_recv()
        total = ishare[swap, 0].astype(F32) + ifar_in[swap, 0].astype(F32) + ifar_in[swap, 1].astype(F32)
        isum[swap] = total.astype(BF16)
        for far in (2, 1, 3):
            image_near(swap, far).start()

    def weight_rows_of(i):
        chip = order_of(i)
        g_passed(chip)
        at = rows(chip * 256, 256)
        g = gbuf[pl.ds(2 * chip, 2)].reshape(256, 512)
        out_part = dot_tn(g, act[at, :])
        pre_grad = (dot_nt(g, wo_all[0, core]) * slope[at, :]).astype(BF16)
        in_part = dot_nn(hin_t[:, at], pre_grad)

        @pl.when(i == 0)
        def _():
            wacc[1] = out_part
            wacc[0] = in_part

        @pl.when(i > 0)
        def _():
            wacc[1] += out_part
            wacc[0] += in_part

    def weight_step(i):
        @pl.when(i < 4)
        def _():
            pl.when(i % 2 == 1)(lambda: g_arrive(order_of(i)))
            pl.when(i != 2)(lambda: g_pass(i).start())

        @pl.when(i == 4)
        def _():
            loop(8, lambda k: in_copy(k).start(), 1)
            inbuf[me] = gin[section]

        @pl.when(i == 2)
        def _():
            for swap in both:
                image_fold(swap)

        pl.when(i > 0)(lambda: weight_rows_of(i - 1))

    for half in both:
        q = (3 - x) * 2 + core
        block = gbuf.at[q, pl.ds(half * 64, 64)]
        copy_to(block, block, gf_ss.at[0], g_rs.at[q * 2 + half], line(me)).wait_recv()
        g_forward(half).start()
    g_pass(2).start()
    loop(5, weight_step)

    def put_weight(which, value):
        for zz in range(4):
            for yy in range(4):
                block = value[(zz * 4 + yy) * 32 : (zz * 4 + yy + 1) * 32].astype(BF16)
                wg[which, 0, zz, yy] = block[:, :256]
                wg[which, 1, yy, zz] = block[:, 256:]

    def weight_far(which, swap, n):
        first = y if swap else z
        block = wg.at[which, swap]
        landed = wfar_in.at[which, swap]
        src, dst, to = (
            (block.at[(first + 2) % 4, 0:2], wrelay_in.at[which, swap, 0], 1),
            (block.at[(first + 2) % 4, 2:4], wrelay_in.at[which, swap, 1], 3),
            (block.at[(first + 1) % 4, 2:4], landed.at[0, 2:4], 1),
            (block.at[(first + 3) % 4, 0:2], landed.at[1, 0:2], 3),
            (wjoined.at[which, swap, 0], landed.at[0, 0:2], 1),
            (wjoined.at[which, swap, 1], landed.at[1, 2:4], 3),
        )[n]
        k = which * 12 + swap * 6 + n
        return copy_to(src, dst, wf_ss.at[k], wf_rs.at[k], step_of(swap, to))

    def weight_relay(which):
        for n, far, lo in ((0, 1, 0), (1, 3, 2)):
            for swap in both:
                weight_far(which, swap, n).wait_recv()
                block = wg[which, swap, ((y if swap else z) + far) % 4, lo : lo + 2]
                wjoined[which, swap, n] = (
                    block.astype(F32) + wrelay_in[which, swap, n].astype(F32)
                ).astype(BF16)
                weight_far(which, swap, n + 4).start()

    def weight_near(which, swap, far):
        n = which * 6 + swap * 3 + 3 - far
        at = ((z if swap else y) + far) % 4
        return copy_to(
            wsum.at[which, swap, at], wnear_in.at[which, swap, 3 - far], wn_ss.at[n], wn_rs.at[n], step_of(1 - swap, far)
        )

    def weight_start(which, messages):
        for n in messages:
            for swap in both:
                weight_far(which, swap, n).start()

    def weight_fold(which):
        for swap in both:
            for n in range(2, 6):
                weight_far(which, swap, n).wait_recv()
            total = wg[which, swap, y if swap else z].astype(F32)
            for side in both:
                total = total + wfar_in[which, swap, side].astype(F32)
            wsum[which, swap] = total.astype(BF16)
        for far in (2, 1, 3):
            for swap in both:
                weight_near(which, swap, far).start()

    def weight_end(which, out):
        for swap in both:
            total = wsum[which, swap, z if swap else y].astype(F32)
            for far in (1, 2, 3):
                landed = wnear_in.at[which, swap, far - 1]
                n = which * 6 + swap * 3 + far - 1
                copy_to(landed, landed, wn_ss.at[n], wn_rs.at[n], {"dp": dp}).wait_recv()
                total = total + landed[...].astype(F32)
            out[0, :, swap * 256 : (swap + 1) * 256] = total

    put_weight(1, wacc[1])
    weight_start(1, (0, 1))
    put_weight(0, wacc[0])
    weight_start(0, (0, 1))
    weight_start(1, (2, 3))
    weight_start(0, (2, 3))

    weight_relay(1)
    weight_relay(0)
    for swap in both:
        total = isum[swap, 0].astype(F32)
        for far in (1, 2, 3):
            landed = inear_in.at[swap, far - 1]
            copy_to(landed, landed, ir_ss.at[0], ir_rs.at[swap * 3 + far - 1], {"dp": dp}).wait_recv()
            total = total + landed[...].astype(F32)
        ifull[:, swap * 256 : (swap + 1) * 256] = total.T
    total = ifull[...] * mult
    image_unit, image_len = unit_rows(image[...])
    ihalf[0] = unit_backward(image_unit, image_len, total).astype(BF16)
    ihalf_copy = copy_to(ihalf.at[0], ihalf.at[1], ih_s.at[0], ih_s.at[1], line(twin))
    ihalf_copy.start()
    weight_fold(1)

    def in_wait(i):
        q = (me + i) % 8
        copy_to(gin.at[0], inbuf.at[q], in_ss.at[i], in_rs.at[q], line(me)).wait_recv()

    loop(8, in_wait, 1)
    input_out[...] = inbuf[...].reshape(1024, 256)

    weight_fold(0)
    image_out[rows(section * 128), :] = ihalf[0]
    ihalf_copy.wait_recv()
    image_out[rows((1 - section) * 128), :] = ihalf[1]
    weight_end(1, second_out)
    weight_end(0, first_out)
    for copy in sends:
        copy.wait_send()
    h_copy.wait_send()
    for n in range(6):
        wx(n, *wx_plan[n]).wait_send()
    for which in both:
        for j in range(4):
            wy(which, j).wait_send()
        for j in range(-1, 5):
            wd(which, j, core).wait_send()
    for k in range(1, 16):
        cst_copy(k).wait_send()
    loop(8, lambda i: rst_copy(i).wait_send(), 1)
    loop(4, lambda i: pass_copy(i).wait_send())
    loop(4, lambda i: tshare_copy((x + i) % 4).wait_send(), 1)
    for swap in both:
        for far in (1, 2, 3):
            image_near(swap, far).wait_send()
        for n in range(6):
            image_far(n, swap).wait_send()
    ihalf_copy.wait_send()
    for layer, sems in ((1, g1_ss), (0, g0_ss)):
        for half in both:
            g_copy(layer, half, sems).wait_send()
    for half in both:
        g_forward(half).wait_send()
    loop(4, lambda i: g_pass(i).wait_send())
    loop(8, lambda i: in_copy(i).wait_send(), 1)
    for which in both:
        for swap in both:
            for far in (1, 2, 3):
                weight_near(which, swap, far).wait_send()
            for n in range(6):
                weight_far(which, swap, n).wait_send()


def settle(*refs):
    for src, dst in zip(refs[:4], refs[4:]):
        dst[...] = src[...]


def body(text_feats, image_feats, logit_scale, layer_inputs, w_in, w_out):
    vmem = pl.BlockSpec(memory_space=pltpu.VMEM)
    dma = pltpu.SemaphoreType.DMA
    scratch = [
        pltpu.VMEM((1024, 512), BF16),
        pltpu.VMEM((128, 512), BF16),
        pltpu.VMEM((1024, 512), BF16),
        pltpu.VMEM((16, 128, 512), BF16),
        pltpu.VMEM((1024, 512), BF16),
        pltpu.VMEM((512, 1024), BF16),
        pltpu.VMEM((8, 1024, 256), F32),
        *[pltpu.VMEM((256, 2048), BF16)] * 4,
        pltpu.VMEM((1024, 128), F32),
        pltpu.VMEM((1024, 128), F32),
        pltpu.VMEM((1024, 128), F32),
        pltpu.VMEM((8, 128), F32),
        pltpu.VMEM((8, 8, 128), F32),
        pltpu.VMEM((8, 128), F32),
        pltpu.VMEM((16, 128), F32),
        pltpu.VMEM((16, 128), F32),
        pltpu.VMEM((16, 16, 128), F32),
        pltpu.VMEM((16, 128), F32),
        pltpu.VMEM((8, 128, 512), BF16),
        pltpu.VMEM((4, 128, 512), BF16),
        pltpu.VMEM((4, 128, 512), BF16),
        pltpu.VMEM((2, 4, 4, 256, 128), BF16),
        pltpu.VMEM((2, 2, 2, 256, 128), BF16),
        pltpu.VMEM((2, 2, 2, 256, 128), BF16),
        pltpu.VMEM((2, 2, 4, 256, 128), BF16),
        pltpu.VMEM((2, 4, 256, 128), BF16),
        pltpu.VMEM((2, 3, 256, 128), BF16),
        pltpu.VMEM((128, 512), F32),
        pltpu.VMEM((2, 128, 512), BF16),
        pltpu.VMEM((4, 2, 512, 512), BF16),
        pltpu.VMEM((4, 2, 512, 512), BF16),
        pltpu.VMEM((128, 512), BF16),
        pltpu.VMEM((1024, 512), BF16),
        pltpu.VMEM((1024, 512), F32),
        pltpu.VMEM((8, 128, 512), F32),
        pltpu.VMEM((512, 1024), BF16),
        pltpu.VMEM((8, 128, 512), BF16),
        pltpu.VMEM((2, 128, 256), BF16),
        pltpu.VMEM((2, 128, 512), BF16),
        pltpu.VMEM((8, 128, 256), BF16),
        pltpu.VMEM((2, 512, 512), F32),
        pltpu.VMEM((2, 2, 4, 4, 32, 256), BF16),
        pltpu.VMEM((2, 2, 2, 2, 32, 256), BF16),
        pltpu.VMEM((2, 2, 2, 2, 32, 256), BF16),
        pltpu.VMEM((2, 2, 2, 4, 32, 256), BF16),
        pltpu.VMEM((2, 2, 4, 32, 256), BF16),
        pltpu.VMEM((2, 2, 3, 32, 256), BF16),
        dma((5,)),
        dma((32,)), dma((64,)),
        dma((6,)), dma((8,)), dma((8,)), dma((8,)), dma((12,)), dma((12,)),
        dma((2,)),
        dma((8,)), dma((8,)),
        dma((16,)), dma((16,)),
        dma((4,)), dma((4,)), dma((4,)), dma((4,)),
        dma((12,)), dma((12,)), dma((6,)), dma((6,)),
        dma((2,)),
        dma((2,)), dma((2,)), dma((2,)), dma((16,)), dma((4,)), dma((4,)),
        dma((8,)), dma((8,)),
        dma((24,)), dma((24,)), dma((12,)), dma((12,)),
    ]
    results = pl.pallas_call(
        kernel,
        out_shape=(
            jax.ShapeDtypeStruct((256, 512), BF16),
            jax.ShapeDtypeStruct((1024, 256), BF16),
            jax.ShapeDtypeStruct((1, 32, 512), F32),
            jax.ShapeDtypeStruct((1, 32, 512), F32),
        ),
        in_specs=[pl.BlockSpec(memory_space=pltpu.SMEM)] + [pl.BlockSpec(memory_space=pl.ANY)] * 5,
        out_specs=(vmem,) * 4,
        scratch_shapes=scratch,
        compiler_params=pltpu.CompilerParams(
            collective_id=0, has_side_effects=True, vmem_limit_bytes=56 * 1024 * 1024
        ),
    )(logit_scale, text_feats, image_feats, layer_inputs, w_in, w_out)
    return pl.pallas_call(
        settle,
        out_shape=tuple(jax.ShapeDtypeStruct(r.shape, r.dtype) for r in results),
        in_specs=[vmem] * 4,
        out_specs=(vmem,) * 4,
    )(*results)


def solution(mesh):
    placed = (
        P("dp", None),
        P(("dp", "mp"), None),
        P(),
        P("section", "dp", None),
        P("section", None, "mp"),
        P("section", "mp", None),
    )
    return jax.shard_map(
        body,
        mesh=mesh,
        in_specs=placed,
        out_specs=(
            P(("dp", "mp"), None),
            P("dp", "section"),
            P("section", "dp", "mp"),
            P("section", "dp", "mp"),
        ),
        check_vma=False,
    )
```

```python
import functools

import jax
import jax.numpy as jnp
from jax import lax
from jax.experimental import pallas as pl
from jax.experimental.pallas import tpu as pltpu
from jax.sharding import PartitionSpec as P

MESH = pl.DeviceIdType.MESH
F32 = jnp.float32
BF16 = jnp.bfloat16
LOW = -1e30
LOG2E = 1.4426950408889634
AROUND = ((0, 1), (0, 3), (1, 0), (3, 0))
ORDER = (
    (0, 0), (0, 1), (0, 3), (1, 0), (3, 0), (1, 1), (1, 3), (3, 1),
    (3, 3), (0, 2), (2, 0), (1, 2), (3, 2), (2, 1), (2, 3), (2, 2),
)


def dot_nt(a, b):
    return lax.dot_general(a, b, (((1,), (1,)), ((), ())), preferred_element_type=F32)


def dot_nn(a, b):
    return lax.dot_general(a, b, (((1,), (0,)), ((), ())), preferred_element_type=F32)


def dot_tn(a, b):
    return lax.dot_general(a, b, (((0,), (0,)), ((), ())), preferred_element_type=F32)


def unit_rows(values):
    wide = values.astype(F32)
    length = jnp.sqrt(jnp.sum(wide * wide, axis=1, keepdims=True) + 1.0)
    return wide / length, length


def unit_backward(unit, length, grad):
    return (grad - unit * jnp.sum(unit * grad, axis=1, keepdims=True)) / length


def slope_of(pre):
    s = jax.nn.sigmoid(1.702 * pre)
    return s + 1.702 * pre * s * (1.0 - s)


def rows(start, size=128):
    return pl.ds(pl.multiple_of(start, 128), size)


def copy_to(src, dst, send, recv, device):
    return pltpu.make_async_remote_copy(
        src_ref=src, dst_ref=dst, send_sem=send, recv_sem=recv, device_id=device, device_id_type=MESH
    )


def loop(count, fn, start=0):
    def step(i, _):
        fn(i)
        return 0

    lax.fori_loop(start, count, step, 0)


def kernel(
    scale, text_hbm, image_hbm, hin_hbm, win_hbm, wout_hbm,
    image_out, input_out, first_out, second_out,
    text, image, hin,
    cols, tlow, tlow_t, scores, grads0, grads1, grads2, grads3, row_m, row_s, row_a,
    rst, rst_in, rst_a, own_stat, cst, cst_in, col_b,
    tshare, tpass, tshare_in, ishare, relay_in, joined, ifar_in, isum, inear_in, ifull, ihalf,
    wi_all, wo_all, hother, act, slope, slope_own, hin_t, gbuf, gin, gown, inbuf,
    wacc, wg, wrelay_in, wjoined, wfar_in, wsum, wnear_in,
    load_s, cols_ss, cols_rs, wx_ss, wx_rs, wy_ss, wy_rs, wd_ss, wd_rs, h_s, rst_ss, rst_rs, cst_ss, cst_rs,
    tp_ss, tp_rs, ts_ss, ts_rs, if_ss, if_rs, ir_ss, ir_rs, ih_s,
    g1_ss, g0_ss, gf_ss, g_rs, gp_ss, gp_rs, in_ss, in_rs,
    wf_ss, wf_rs, wn_ss, wn_rs,
):
    section = lax.axis_index("section")
    dp = lax.axis_index("dp")
    mp = lax.axis_index("mp")
    me = section * 4 + mp
    x, core = me // 2, me % 2
    z, y = dp // 4, dp % 4
    mult = scale[0]
    mult2 = mult * LOG2E

    def line(q):
        return {"section": q // 4, "mp": q % 4}

    def plane(dz, dy):
        return ((z + dz) % 4) * 4 + (y + dy) % 4

    def slot(dz, dy):
        return ORDER.index((dz % 4, dy % 4))

    def away(k):
        return plane(k // 4, k % 4)

    sends = []

    loads = [
        pltpu.make_async_copy(src, dst, load_s.at[n])
        for n, (src, dst) in enumerate(
            (
                (image_hbm.at[rows(section * 128)], image),
                (text_hbm, text),
                (win_hbm.at[0], wi_all.at[0, core]),
                (wout_hbm.at[0], wo_all.at[0, core]),
                (hin_hbm.at[0], hin),
            )
        )
    ]
    for load in loads:
        load.start()

    barrier = pltpu.get_barrier_semaphore()

    def greet_plane(k):
        pl.semaphore_signal(barrier, inc=1, device_id={"dp": away(k)}, device_id_type=MESH)

    def greet_line(i):
        pl.semaphore_signal(barrier, inc=1, device_id=line((me + i) % 8), device_id_type=MESH)

    loop(16, greet_plane, 1)
    loop(8, greet_line, 1)

    loads[0].wait()
    image_unit, image_len = unit_rows(image[...])
    cols[0] = image_unit.astype(BF16)

    def text_block(r):
        unit, _ = unit_rows(text[rows(r * 128), :])
        low = unit.astype(BF16)
        tlow[rows(r * 128), :] = low
        tlow_t[:, rows(r * 128)] = low.astype(F32).T.astype(BF16)
        row_m[rows(r * 128), :] = jnp.full((128, 128), LOW, F32)
        row_s[rows(r * 128), :] = jnp.zeros((128, 128), F32)

    pl.semaphore_wait(barrier, 22)

    def ag_send(dz, dy, lo, size, ez, ey):
        there = slot(dz - ez, dy - ey)
        copy = copy_to(
            cols.at[slot(dz, dy), lo : lo + size],
            cols.at[there, lo : lo + size],
            cols_ss.at[len(sends)],
            cols_rs.at[there * 4 + lo // 32],
            {"dp": plane(ez, ey)},
        )
        copy.start()
        sends.append(copy)

    def ag_wait(dz, dy, lo, size):
        here = slot(dz, dy)
        block = cols.at[here, lo : lo + size]
        copy_to(block, block, cols_ss.at[0], cols_rs.at[here * 4 + lo // 32], {"dp": dp}).wait_recv()

    def flip(swap, *pair):
        return pair[::-1] if swap else pair

    def half_send(swap, first, second, to_first, to_second, lo=0, size=64):
        dz, dy = flip(swap, first, second)
        ez, ey = flip(swap, to_first, to_second)
        ag_send(dz, dy, lo + 64 * swap, size, ez, ey)

    def half_wait(swap, first, second, lo=0, size=64):
        dz, dy = flip(swap, first, second)
        ag_wait(dz, dy, lo + 64 * swap, size)

    for to in ((0, 1), (0, 3), (1, 0), (3, 0)):
        for swap in (0, 1):
            half_send(swap, 0, 0, *to)

    right, left, opposite = (x + 1) % 4, (x + 3) % 4, (x + 2) % 4
    weights = (wi_all, wo_all)

    def weight_rows(turn, lo=0, size=256):
        return pl.ds(pl.multiple_of((y + z + turn) % 2 * 256 + lo, 64), size)

    def wx(n, which, src, dst, chip):
        at = weight_rows(0)
        ref = weights[which]
        return copy_to(
            ref.at[src, core, at], ref.at[dst, core, at], wx_ss.at[n], wx_rs.at[which * 4 + dst], line(chip * 2 + core)
        )

    wx_plan = ((0, 0, 2, right), (1, 0, 1, left), (1, 0, 2, right), (0, 0, 1, left), (0, 2, 3, right), (1, 1, 3, left))

    def wx_wait(which, rel):
        block = weights[which].at[rel, core, weight_rows(0)]
        copy_to(block, block, wx_ss.at[0], wx_rs.at[which * 4 + rel], line(me)).wait_recv()

    def wy_block(part, j, turn):
        which, first, count = ((0, 1, 2), (0, 3, 1), (1, 1, 3))[part]
        return weights[which].at[pl.ds(first, count), core, weight_rows(turn, j * 64, 64)]

    def wy(part, j):
        dz, dy = AROUND[j]
        block = wy_block(part, j, 0)
        n = part * 4 + j
        return copy_to(block, block, wy_ss.at[n], wy_rs.at[n], {"dp": plane(4 - dz, 4 - dy)})

    def wy_wait(part, j):
        block = wy_block(part, j, 1)
        n = part * 4 + j
        copy_to(block, block, wy_ss.at[n], wy_rs.at[n], {"dp": dp}).wait_recv()

    def wd(which, j, side):
        if j < 0:
            block = weights[which].at[0, side]
        else:
            at = weight_rows(0) if j == 4 else weight_rows(1, j * 64, 64)
            block = weights[which].at[pl.ds(1, 3), side, at]
        n = which * 6 + j + 1
        return copy_to(block, block, wd_ss.at[n], wd_rs.at[n], line(x * 2 + 1 - core))

    twin = (1 - section) * 4 + mp
    h_copy = copy_to(hin.at[rows(twin * 128), :], hother, h_s.at[0], h_s.at[1], line(twin))
    for load in loads[2:]:
        load.wait()
    for n in range(4):
        wx(n, *wx_plan[n]).start()
    for which in (0, 1):
        wd(which, -1, core).start()
    h_copy.start()

    def score_pair(p):
        pair = cols[pl.ds(2 * p, 2)].reshape(256, 512)
        part = dot_nt(tlow[...], pair)
        c_m, c_s = jnp.full((8, 256), LOW, F32), jnp.zeros((8, 256), F32)
        for r in range(8):
            at = slice(r * 128, (r + 1) * 128)
            s = part[at] * mult2
            scores[p, at, :] = s
            s3 = s.reshape(16, 8, 256)
            n_m = jnp.maximum(c_m, jnp.max(s3, axis=0))
            c_s = c_s * jnp.exp2(c_m - n_m) + jnp.sum(jnp.exp2(s3 - n_m[None]), axis=0)
            c_m = n_m
            old = row_m[at, :]
            s0, s1 = s[:, :128], s[:, 128:]
            new = jnp.maximum(old, jnp.maximum(s0, s1))
            row_s[at, :] = row_s[at, :] * jnp.exp2(old - new) + jnp.exp2(s0 - new) + jnp.exp2(s1 - new)
            row_m[at, :] = new

        peak = jnp.max(c_m, axis=0, keepdims=True)
        total = peak + jnp.log2(jnp.sum(c_s * jnp.exp2(c_m - peak), axis=0, keepdims=True))
        for j in (0, 1):
            own_stat[pl.ds(2 * p + j, 1), :] = total[:, j * 128 : (j + 1) * 128]

    def spread(swap, first, second):
        for to in (1, 3):
            half_send(swap, first, second, to, 0)

    both = (0, 1)
    loads[1].wait()
    loop(8, text_block)
    for swap in both:
        half_wait(swap, 0, 1)
        half_wait(swap, 0, 3)
        half_send(swap, 0, 1, 0, 3, 0, 32)
        half_send(swap, 0, 3, 0, 1, 32, 32)
    for swap in both:
        spread(swap, 0, 1)
        spread(swap, 0, 3)
    for swap in both:
        half_wait(swap, 1, 0)
        half_send(swap, 1, 0, 3, 0)
        half_wait(swap, 3, 0)
    loop(2, score_pair)
    for swap in both:
        half_wait(swap, 0, 2, 0, 32)
        half_wait(swap, 0, 2, 32, 32)
        spread(swap, 0, 2)
    for swap in both:
        for second in (1, 3):
            half_wait(swap, 3, second)
            half_send(swap, 3, second, 1, 0)
            half_wait(swap, 1, second)
    wx_wait(0, 2)
    wx(4, *wx_plan[4]).start()
    wx_wait(1, 1)
    wx(5, *wx_plan[5]).start()
    loop(4, score_pair, 2)
    for swap in both:
        half_wait(swap, 2, 0)
    loop(5, score_pair, 4)
    for swap in both:
        half_wait(swap, 1, 2)
        half_send(swap, 1, 2, 3, 0)
        half_wait(swap, 3, 2)
    half_wait(1, 2, 1)
    loop(6, score_pair, 5)
    half_wait(0, 2, 1)
    for swap in both:
        half_wait(swap, 2, 3)
    wx_wait(0, 1)
    for j in range(4):
        wy(0, j).start()
    loop(7, score_pair, 6)
    for swap in both:
        half_wait(swap, 2, 2)
    score_pair(7)
    for k, (dz, dy) in enumerate(ORDER):
        cst[pl.ds(plane(dz, dy), 1), :] = own_stat[k : k + 1, :]

    def cst_copy(k):
        dz, dy = ORDER[k]
        return copy_to(cst, cst_in.at[dp], cst_ss.at[k], cst_rs.at[dp], {"dp": plane(dz, dy)})

    def cst_wait(k):
        copy_to(cst, cst_in.at[away(k)], cst_ss.at[k], cst_rs.at[away(k)], {"dp": dp}).wait_recv()

    for k in range(15, 0, -1):
        cst_copy(k).start()
    cst_in[dp] = cst[...]

    for r in range(8):
        m_t = row_m[r * 128 : (r + 1) * 128, :].T
        s_t = row_s[r * 128 : (r + 1) * 128, :].T
        peak = jnp.max(m_t, axis=0, keepdims=True)
        rst[r : r + 1, :] = peak + jnp.log2(jnp.sum(s_t * jnp.exp2(m_t - peak), axis=0, keepdims=True))

    def rst_copy(i):
        q = (me + i) % 8
        return copy_to(rst, rst_in.at[me], rst_ss.at[i], rst_rs.at[me], line(q))

    def rst_wait(i):
        q = (me + i) % 8
        copy_to(rst, rst_in.at[q], rst_ss.at[i], rst_rs.at[q], line(me)).wait_recv()

    loop(8, lambda i: rst_copy(i).start(), 1)
    rst_in[me] = rst[...]

    def hidden_block(r):
        at = rows(r * 128)
        h = hin[at, :]
        pre = dot_nn(h, wi_all[0, core])
        sig = jax.nn.sigmoid(1.702 * pre)
        act[at, :] = (pre * sig).astype(BF16)
        slope[at, :] = sig + 1.702 * pre * sig * (1.0 - sig)
        hin_t[:, at] = h.astype(F32).T.astype(BF16)

    loop(8, hidden_block)

    loop(8, rst_wait, 1)
    peak = jnp.max(rst_in[...], axis=0)
    total = jnp.sum(jnp.exp2(rst_in[...] - peak[None]), axis=0)
    rst_a[...] = peak + jnp.log2(2.0 * total)
    for r in range(8):
        row_a[r * 128 : (r + 1) * 128, :] = jnp.broadcast_to(rst_a[r : r + 1, :], (128, 128)).T

    loop(16, cst_wait, 1)
    peak = jnp.max(cst_in[...], axis=0)
    total = jnp.sum(jnp.exp2(cst_in[...] - peak[None]), axis=0)
    own_stat[...] = peak + jnp.log2(2.0 * total)
    for k, (dz, dy) in enumerate(ORDER):
        col_b[k : k + 1, :] = own_stat[pl.ds(plane(dz, dy), 1), :]

    def pass_copy(chip):
        other = chip * 2 + 1 - core
        return copy_to(tshare.at[other], tpass.at[chip], tp_ss.at[chip], tp_rs.at[chip], line(x * 2 + 1 - core))

    def tshare_copy(chip):
        own = chip * 2 + core
        return copy_to(tshare.at[own], tshare_in.at[x], ts_ss.at[chip], ts_rs.at[x], line(own))

    chips = (opposite, right, left, x)
    parts = (grads0, grads1, grads2, grads3)
    mine = 2 * mp + section
    eye = (
        lax.broadcasted_iota(jnp.int32, (128, 128), 0) == lax.broadcasted_iota(jnp.int32, (128, 128), 1)
    ).astype(F32)

    def make_grads(i):
        for half in both:
            at = rows(chips[i] * 256 + half * 128)
            a = row_a[at, :]
            for k in range(16):
                p, j = k // 2, k % 2
                s = scores[p, at, j * 128 : (j + 1) * 128]
                part = jnp.exp2(s - a) + jnp.exp2(s - col_b[k : k + 1, :])
                if k == 0:
                    part = part - eye * jnp.where(chips[i] * 2 + half == mine, 1.0, 0.0)
                parts[i][half * 128 : (half + 1) * 128, k * 128 : (k + 1) * 128] = part.astype(BF16)

    def text_merge(chip):
        own = chip * 2 + core
        pass_copy(chip).wait_recv()
        tshare[own] = (tshare[own].astype(F32) + tpass[chip].astype(F32)).astype(BF16)

    def wd_pass(which):
        for j in range(4):
            for part in ((0, 1), (2,))[which]:
                wy_wait(part, j)
            wd(which, j, core).start()

    def wd_wait(which):
        for j in range(-1, 5):
            wd(which, j, 1 - core).wait_recv()

    wx_wait(1, 2)
    for which in both:
        wx_wait(which, 3)
    for part in (1, 2):
        for j in range(4):
            wy(part, j).start()
    for which in both:
        wd(which, 4, core).start()
    make_grads(0)
    for i in range(4):
        if i < 3:
            make_grads(i + 1)
        part = dot_nn(parts[i][...], cols[...].reshape(2048, 512))
        for j in (0, 1):
            tshare[chips[i] * 2 + j] = part[j * 128 : (j + 1) * 128].astype(BF16)
        pass_copy(chips[i]).start()
        if i > 0:
            text_merge(chips[i - 1])
            tshare_copy(chips[i - 1]).start()
    text_merge(x)
    wd_pass(0)

    def image_part(p):
        part = sum(
            dot_nn(tlow_t[:, rows(chips[i] * 256, 256)], parts[i][:, p * 256 : (p + 1) * 256]) for i in range(4)
        )
        for j in (0, 1):
            dz, dy = ORDER[2 * p + j]
            block = part[:, j * 128 : (j + 1) * 128].astype(BF16)
            ishare[0, dz, dy] = block[:256]
            ishare[1, dy, dz] = block[256:]

    def step_of(swap, far):
        return {"dp": plane(*flip(swap, far, 0))}

    def image_far(n, swap):
        src, dst, to = (
            (ishare.at[swap, 2, 0:2], relay_in.at[swap, 0], 1),
            (ishare.at[swap, 2, 2:4], relay_in.at[swap, 1], 3),
            (ishare.at[swap, 1, 2:4], ifar_in.at[swap, 0, 2:4], 1),
            (ishare.at[swap, 3, 0:2], ifar_in.at[swap, 1, 0:2], 3),
            (joined.at[swap, 0], ifar_in.at[swap, 0, 0:2], 1),
            (joined.at[swap, 1], ifar_in.at[swap, 1, 2:4], 3),
        )[n]
        k = swap * 6 + n
        return copy_to(src, dst, if_ss.at[k], if_rs.at[k], step_of(swap, to))

    def image_near(swap, far):
        n = swap * 3 + 3 - far
        return copy_to(isum.at[swap, far], inear_in.at[swap, 3 - far], ir_ss.at[n], ir_rs.at[n], step_of(1 - swap, far))

    for p in range(7, -1, -1):
        image_part(p)
    for n in range(4):
        for swap in both:
            image_far(n, swap).start()

    def image_relay():
        for n, far, lo in ((0, 1, 0), (1, 3, 2)):
            for swap in both:
                image_far(n, swap).wait_recv()
                joined[swap, n] = (
                    ishare[swap, far, lo : lo + 2].astype(F32) + relay_in[swap, n].astype(F32)
                ).astype(BF16)
                image_far(n + 4, swap).start()


    wd_pass(1)
    h_copy.wait_recv()

    wd_wait(0)

    def home(q):
        turn = (q // 2 + 4 - x) % 4
        return jnp.where(turn == 2, 3, jnp.where(turn == 3, 2, turn)), q % 2

    def own_block(r):
        h = jnp.where(r // 4 == section, hin[rows(me * 128), :], hother[...])
        slope_own[r] = slope_of(dot_nn(h, wi_all[home(r)]))

    loop(8, own_block, 4)

    def tshare_sum(i, acc):
        chip = (x + i) % 4
        copy_to(tshare.at[0], tshare_in.at[chip], ts_ss.at[chip], ts_rs.at[chip], line(me)).wait_recv()
        return acc + tshare_in[chip].astype(F32)

    total = lax.fori_loop(1, 4, tshare_sum, tshare[me].astype(F32)) * mult
    unit, length = unit_rows(text[rows(me * 128), :])
    gown[0] = unit_backward(unit, length, total).astype(BF16)

    sibling = x + 1 - 2 * (x % 2)

    def g_copy(layer, half, sems):
        at = pl.ds(half * 64, 64)
        to = jnp.where(section == layer, sibling, 3 - x) * 2 + core
        return copy_to(gown.at[1 - layer, at], gbuf.at[me, at], sems.at[half], g_rs.at[me * 2 + half], line(to))

    def g_send(layer, sems):
        for half in both:
            g_copy(layer, half, sems).start()

        @pl.when(section == layer)
        def _():
            gbuf[me] = gown[1 - layer]

    def g_forward(half):
        q = (3 - x) * 2 + core
        block = gbuf.at[q, pl.ds(half * 64, 64)]
        return copy_to(block, block, gf_ss.at[half], g_rs.at[q * 2 + half], line(sibling * 2 + core))

    def g_arrive(chip):
        q = chip * 2 + core
        for half in both:
            block = gbuf.at[q, pl.ds(half * 64, 64)]
            copy_to(block, block, gf_ss.at[0], g_rs.at[q * 2 + half], line(me)).wait_recv()

    def order_of(i):
        return jnp.where(i == 0, x, jnp.where(i == 1, sibling, jnp.where(i == 2, 3 - x, 3 - sibling)))

    def g_pass(i):
        chip = order_of(i)
        block = gbuf.at[chip * 2 + core]
        return copy_to(block, block, gp_ss.at[i], gp_rs.at[chip], line(x * 2 + 1 - core))

    def g_passed(chip):
        block = gbuf.at[chip * 2 + 1 - core]
        copy_to(block, block, gp_ss.at[0], gp_rs.at[chip], line(me)).wait_recv()

    def chain(layer):
        g = gown[1 - layer]

        def step(j, acc):
            q = layer * 4 + j
            back = dot_nt(g, wo_all[home(q)])
            pre_grad = (back * slope_own[q]).astype(BF16)
            return acc + dot_nt(pre_grad, wi_all[home(q)])

        return lax.fori_loop(0, 4, step, g.astype(F32)).astype(BF16)

    wd_wait(1)
    g_send(1, g1_ss)
    gown[1] = chain(1)
    g_send(0, g0_ss)
    loop(4, own_block)
    image_relay()
    lowest = chain(0)
    gin[0] = lowest[:, :256]
    gin[1] = lowest[:, 256:]

    def in_copy(i):
        q = (me + i) % 8
        return copy_to(gin.at[q // 4], inbuf.at[me], in_ss.at[i], in_rs.at[me], line(q))

    def image_fold(swap):
        for n in range(2, 6):
            image_far(n, swap).wait_recv()
        total = ishare[swap, 0].astype(F32) + ifar_in[swap, 0].astype(F32) + ifar_in[swap, 1].astype(F32)
        isum[swap] = total.astype(BF16)
        for far in (2, 1, 3):
            image_near(swap, far).start()

    def weight_rows_of(i):
        chip = order_of(i)
        g_passed(chip)
        at = rows(chip * 256, 256)
        g = gbuf[pl.ds(2 * chip, 2)].reshape(256, 512)
        out_part = dot_tn(g, act[at, :])
        pre_grad = (dot_nt(g, wo_all[0, core]) * slope[at, :]).astype(BF16)
        in_part = dot_nn(hin_t[:, at], pre_grad)

        @pl.when(i == 0)
        def _():
            wacc[1] = out_part
            wacc[0] = in_part

        @pl.when(i > 0)
        def _():
            wacc[1] += out_part
            wacc[0] += in_part

    def weight_step(i):
        @pl.when(i < 4)
        def _():
            pl.when(i % 2 == 1)(lambda: g_arrive(order_of(i)))
            pl.when(i != 2)(lambda: g_pass(i).start())

        @pl.when(i == 4)
        def _():
            loop(8, lambda k: in_copy(k).start(), 1)
            inbuf[me] = gin[section]

        @pl.when(i == 2)
        def _():
            for swap in both:
                image_fold(swap)

        pl.when(i > 0)(lambda: weight_rows_of(i - 1))

    for half in both:
        q = (3 - x) * 2 + core
        block = gbuf.at[q, pl.ds(half * 64, 64)]
        copy_to(block, block, gf_ss.at[0], g_rs.at[q * 2 + half], line(me)).wait_recv()
        g_forward(half).start()
    g_pass(2).start()
    loop(5, weight_step)

    def put_weight(which, value):
        for zz in range(4):
            for yy in range(4):
                block = value[(zz * 4 + yy) * 32 : (zz * 4 + yy + 1) * 32].astype(BF16)
                wg[which, 0, zz, yy] = block[:, :256]
                wg[which, 1, yy, zz] = block[:, 256:]

    def weight_far(which, swap, n):
        first = y if swap else z
        block = wg.at[which, swap]
        landed = wfar_in.at[which, swap]
        src, dst, to = (
            (block.at[(first + 2) % 4, 0:2], wrelay_in.at[which, swap, 0], 1),
            (block.at[(first + 2) % 4, 2:4], wrelay_in.at[which, swap, 1], 3),
            (block.at[(first + 1) % 4, 2:4], landed.at[0, 2:4], 1),
            (block.at[(first + 3) % 4, 0:2], landed.at[1, 0:2], 3),
            (wjoined.at[which, swap, 0], landed.at[0, 0:2], 1),
            (wjoined.at[which, swap, 1], landed.at[1, 2:4], 3),
        )[n]
        k = which * 12 + swap * 6 + n
        return copy_to(src, dst, wf_ss.at[k], wf_rs.at[k], step_of(swap, to))

    def weight_relay(which):
        for n, far, lo in ((0, 1, 0), (1, 3, 2)):
            for swap in both:
                weight_far(which, swap, n).wait_recv()
                block = wg[which, swap, ((y if swap else z) + far) % 4, lo : lo + 2]
                wjoined[which, swap, n] = (
                    block.astype(F32) + wrelay_in[which, swap, n].astype(F32)
                ).astype(BF16)
                weight_far(which, swap, n + 4).start()

    def weight_near(which, swap, far):
        n = which * 6 + swap * 3 + 3 - far
        at = ((z if swap else y) + far) % 4
        return copy_to(
            wsum.at[which, swap, at], wnear_in.at[which, swap, 3 - far], wn_ss.at[n], wn_rs.at[n], step_of(1 - swap, far)
        )

    def weight_start(which, messages):
        for n in messages:
            for swap in both:
                weight_far(which, swap, n).start()

    def weight_fold(which):
        for swap in both:
            for n in range(2, 6):
                weight_far(which, swap, n).wait_recv()
            total = wg[which, swap, y if swap else z].astype(F32)
            for side in both:
                total = total + wfar_in[which, swap, side].astype(F32)
            wsum[which, swap] = total.astype(BF16)
        for far in (2, 1, 3):
            for swap in both:
                weight_near(which, swap, far).start()

    def weight_end(which, out):
        for swap in both:
            total = wsum[which, swap, z if swap else y].astype(F32)
            for far in (1, 2, 3):
                landed = wnear_in.at[which, swap, far - 1]
                n = which * 6 + swap * 3 + far - 1
                copy_to(landed, landed, wn_ss.at[n], wn_rs.at[n], {"dp": dp}).wait_recv()
                total = total + landed[...].astype(F32)
            out[0, :, swap * 256 : (swap + 1) * 256] = total

    put_weight(1, wacc[1])
    weight_start(1, (0, 1))
    put_weight(0, wacc[0])
    weight_start(0, (0, 1))
    weight_start(1, (2, 3))
    weight_start(0, (2, 3))

    weight_relay(1)
    weight_relay(0)
    for swap in both:
        total = isum[swap, 0].astype(F32)
        for far in (1, 2, 3):
            landed = inear_in.at[swap, far - 1]
            copy_to(landed, landed, ir_ss.at[0], ir_rs.at[swap * 3 + far - 1], {"dp": dp}).wait_recv()
            total = total + landed[...].astype(F32)
        ifull[:, swap * 256 : (swap + 1) * 256] = total.T
    total = ifull[...] * mult
    image_unit, image_len = unit_rows(image[...])
    ihalf[0] = unit_backward(image_unit, image_len, total).astype(BF16)
    ihalf_copy = copy_to(ihalf.at[0], ihalf.at[1], ih_s.at[0], ih_s.at[1], line(twin))
    ihalf_copy.start()
    weight_fold(1)

    def in_wait(i):
        q = (me + i) % 8
        copy_to(gin.at[0], inbuf.at[q], in_ss.at[i], in_rs.at[q], line(me)).wait_recv()

    loop(8, in_wait, 1)
    input_out[...] = inbuf[...].reshape(1024, 256)

    weight_fold(0)
    image_out[rows(section * 128), :] = ihalf[0]
    ihalf_copy.wait_recv()
    image_out[rows((1 - section) * 128), :] = ihalf[1]
    weight_end(1, second_out)
    weight_end(0, first_out)
    for copy in sends:
        copy.wait_send()
    h_copy.wait_send()
    for n in range(6):
        wx(n, *wx_plan[n]).wait_send()
    for which in both:
        for j in range(-1, 5):
            wd(which, j, core).wait_send()
    for part in range(3):
        for j in range(4):
            wy(part, j).wait_send()
    for k in range(1, 16):
        cst_copy(k).wait_send()
    loop(8, lambda i: rst_copy(i).wait_send(), 1)
    loop(4, lambda i: pass_copy(i).wait_send())
    loop(4, lambda i: tshare_copy((x + i) % 4).wait_send(), 1)
    for swap in both:
        for far in (1, 2, 3):
            image_near(swap, far).wait_send()
        for n in range(6):
            image_far(n, swap).wait_send()
    ihalf_copy.wait_send()
    for layer, sems in ((1, g1_ss), (0, g0_ss)):
        for half in both:
            g_copy(layer, half, sems).wait_send()
    for half in both:
        g_forward(half).wait_send()
    loop(4, lambda i: g_pass(i).wait_send())
    loop(8, lambda i: in_copy(i).wait_send(), 1)
    for which in both:
        for swap in both:
            for far in (1, 2, 3):
                weight_near(which, swap, far).wait_send()
            for n in range(6):
                weight_far(which, swap, n).wait_send()


def settle(*refs):
    sems = refs[8]
    copies = [pltpu.make_async_copy(src, dst, sems.at[n]) for n, (src, dst) in enumerate(zip(refs[:4], refs[4:8]))]
    for copy in copies:
        copy.start()
    for copy in copies:
        copy.wait()


def body(text_feats, image_feats, logit_scale, layer_inputs, w_in, w_out):
    vmem = pl.BlockSpec(memory_space=pltpu.VMEM)
    dma = pltpu.SemaphoreType.DMA
    scratch = [
        pltpu.VMEM((1024, 512), BF16),
        pltpu.VMEM((128, 512), BF16),
        pltpu.VMEM((1024, 512), BF16),
        pltpu.VMEM((16, 128, 512), BF16),
        pltpu.VMEM((1024, 512), BF16),
        pltpu.VMEM((512, 1024), BF16),
        pltpu.VMEM((8, 1024, 256), F32),
        *[pltpu.VMEM((256, 2048), BF16)] * 4,
        pltpu.VMEM((1024, 128), F32),
        pltpu.VMEM((1024, 128), F32),
        pltpu.VMEM((1024, 128), F32),
        pltpu.VMEM((8, 128), F32),
        pltpu.VMEM((8, 8, 128), F32),
        pltpu.VMEM((8, 128), F32),
        pltpu.VMEM((16, 128), F32),
        pltpu.VMEM((16, 128), F32),
        pltpu.VMEM((16, 16, 128), F32),
        pltpu.VMEM((16, 128), F32),
        pltpu.VMEM((8, 128, 512), BF16),
        pltpu.VMEM((4, 128, 512), BF16),
        pltpu.VMEM((4, 128, 512), BF16),
        pltpu.VMEM((2, 4, 4, 256, 128), BF16),
        pltpu.VMEM((2, 2, 2, 256, 128), BF16),
        pltpu.VMEM((2, 2, 2, 256, 128), BF16),
        pltpu.VMEM((2, 2, 4, 256, 128), BF16),
        pltpu.VMEM((2, 4, 256, 128), BF16),
        pltpu.VMEM((2, 3, 256, 128), BF16),
        pltpu.VMEM((128, 512), F32),
        pltpu.VMEM((2, 128, 512), BF16),
        pltpu.VMEM((4, 2, 512, 512), BF16),
        pltpu.VMEM((4, 2, 512, 512), BF16),
        pltpu.VMEM((128, 512), BF16),
        pltpu.VMEM((1024, 512), BF16),
        pltpu.VMEM((1024, 512), F32),
        pltpu.VMEM((8, 128, 512), F32),
        pltpu.VMEM((512, 1024), BF16),
        pltpu.VMEM((8, 128, 512), BF16),
        pltpu.VMEM((2, 128, 256), BF16),
        pltpu.VMEM((2, 128, 512), BF16),
        pltpu.VMEM((8, 128, 256), BF16),
        pltpu.VMEM((2, 512, 512), F32),
        pltpu.VMEM((2, 2, 4, 4, 32, 256), BF16),
        pltpu.VMEM((2, 2, 2, 2, 32, 256), BF16),
        pltpu.VMEM((2, 2, 2, 2, 32, 256), BF16),
        pltpu.VMEM((2, 2, 2, 4, 32, 256), BF16),
        pltpu.VMEM((2, 2, 4, 32, 256), BF16),
        pltpu.VMEM((2, 2, 3, 32, 256), BF16),
        dma((5,)),
        dma((32,)), dma((64,)),
        dma((6,)), dma((8,)), dma((12,)), dma((12,)), dma((12,)), dma((12,)),
        dma((2,)),
        dma((8,)), dma((8,)),
        dma((16,)), dma((16,)),
        dma((4,)), dma((4,)), dma((4,)), dma((4,)),
        dma((12,)), dma((12,)), dma((6,)), dma((6,)),
        dma((2,)),
        dma((2,)), dma((2,)), dma((2,)), dma((16,)), dma((4,)), dma((4,)),
        dma((8,)), dma((8,)),
        dma((24,)), dma((24,)), dma((12,)), dma((12,)),
    ]
    results = pl.pallas_call(
        kernel,
        out_shape=(
            pltpu.VMEM((256, 512), BF16),
            pltpu.VMEM((1024, 256), BF16),
            pltpu.VMEM((1, 32, 512), F32),
            pltpu.VMEM((1, 32, 512), F32),
        ),
        in_specs=[pl.BlockSpec(memory_space=pltpu.SMEM)] + [pl.BlockSpec(memory_space=pl.ANY)] * 5,
        out_specs=(vmem,) * 4,
        scratch_shapes=scratch,
        compiler_params=pltpu.CompilerParams(
            collective_id=0, has_side_effects=True, vmem_limit_bytes=54 * 1024 * 1024
        ),
    )(logit_scale, text_feats, image_feats, layer_inputs, w_in, w_out)
    results = [pltpu.with_memory_space_constraint(r, pltpu.VMEM) for r in results]
    return pl.pallas_call(
        settle,
        out_shape=tuple(jax.ShapeDtypeStruct(r.shape, r.dtype) for r in results),
        in_specs=[vmem] * 4,
        out_specs=(pl.BlockSpec(memory_space=pl.ANY),) * 4,
        scratch_shapes=[dma((4,))],
    )(*results)


def solution(mesh):
    placed = (
        P("dp", None),
        P(("dp", "mp"), None),
        P(),
        P("section", "dp", None),
        P("section", None, "mp"),
        P("section", "mp", None),
    )
    return jax.shard_map(
        body,
        mesh=mesh,
        in_specs=placed,
        out_specs=(
            P(("dp", "mp"), None),
            P("dp", "section"),
            P("section", "dp", "mp"),
            P("section", "dp", "mp"),
        ),
        check_vma=False,
    )
```

```python
import functools

import jax
import jax.numpy as jnp
from jax import lax
from jax.experimental import pallas as pl
from jax.experimental.pallas import tpu as pltpu
from jax.sharding import PartitionSpec as P

MESH = pl.DeviceIdType.MESH
F32 = jnp.float32
BF16 = jnp.bfloat16
LOW = -1e30
LOG2E = 1.4426950408889634
AROUND = ((0, 1), (0, 3), (1, 0), (3, 0))
ORDER = (
    (0, 0), (0, 1), (0, 3), (1, 0), (3, 0), (1, 1), (1, 3), (3, 1),
    (3, 3), (0, 2), (2, 0), (1, 2), (3, 2), (2, 1), (2, 3), (2, 2),
)


def dot_nt(a, b):
    return lax.dot_general(a, b, (((1,), (1,)), ((), ())), preferred_element_type=F32)


def dot_nn(a, b):
    return lax.dot_general(a, b, (((1,), (0,)), ((), ())), preferred_element_type=F32)


def dot_tn(a, b):
    return lax.dot_general(a, b, (((0,), (0,)), ((), ())), preferred_element_type=F32)


def unit_rows(values):
    wide = values.astype(F32)
    length = jnp.sqrt(jnp.sum(wide * wide, axis=1, keepdims=True) + 1.0)
    return wide / length, length


def unit_backward(unit, length, grad):
    return (grad - unit * jnp.sum(unit * grad, axis=1, keepdims=True)) / length


def slope_of(pre):
    s = jax.nn.sigmoid(1.702 * pre)
    return s + 1.702 * pre * s * (1.0 - s)


def rows(start, size=128):
    return pl.ds(pl.multiple_of(start, 128), size)


def copy_to(src, dst, send, recv, device):
    return pltpu.make_async_remote_copy(
        src_ref=src, dst_ref=dst, send_sem=send, recv_sem=recv, device_id=device, device_id_type=MESH
    )


def loop(count, fn, start=0):
    def step(i, _):
        fn(i)
        return 0

    lax.fori_loop(start, count, step, 0)


def kernel(
    scale, text_hbm, image_hbm, hin_hbm, win_hbm, wout_hbm,
    image_out, input_out, first_out, second_out,
    text, image, hin,
    cols, tlow, tlow_t, scores, grads0, grads1, grads2, grads3, row_m, row_s, row_a,
    rst, rst_in, rst_a, own_stat, cst, cst_in, col_b,
    tshare, tpass, tshare_in, ishare, relay_in, joined, ifar_in, isum, inear_in, ifull, ihalf,
    wi_all, wo_all, hother, act, slope, slope_own, hin_t, gbuf, gin, gown, inbuf,
    wacc, wg, wrelay_in, wjoined, wfar_in, wsum, wnear_in,
    load_s, cols_ss, cols_rs, wx_ss, wx_rs, wy_ss, wy_rs, wd_ss, wd_rs, h_s, rst_ss, rst_rs, cst_ss, cst_rs,
    tp_ss, tp_rs, ts_ss, ts_rs, if_ss, if_rs, ir_ss, ir_rs, ih_s,
    g1_ss, g0_ss, gf_ss, g_rs, gp_ss, gp_rs, in_ss, in_rs,
    wf_ss, wf_rs, wn_ss, wn_rs,
):
    section = lax.axis_index("section")
    dp = lax.axis_index("dp")
    mp = lax.axis_index("mp")
    me = section * 4 + mp
    x, core = me // 2, me % 2
    z, y = dp // 4, dp % 4
    mult = scale[0]
    mult2 = mult * LOG2E

    def line(q):
        return {"section": q // 4, "mp": q % 4}

    def plane(dz, dy):
        return ((z + dz) % 4) * 4 + (y + dy) % 4

    def slot(dz, dy):
        return ORDER.index((dz % 4, dy % 4))

    def away(k):
        return plane(k // 4, k % 4)

    sends = []

    loads = [
        pltpu.make_async_copy(src, dst, load_s.at[n])
        for n, (src, dst) in enumerate(
            (
                (image_hbm.at[rows(section * 128)], image),
                (text_hbm, text),
                (win_hbm.at[0], wi_all.at[0, core]),
                (wout_hbm.at[0], wo_all.at[0, core]),
                (hin_hbm.at[0], hin),
            )
        )
    ]
    for load in loads:
        load.start()

    barrier = pltpu.get_barrier_semaphore()

    def greet_plane(k):
        pl.semaphore_signal(barrier, inc=1, device_id={"dp": away(k)}, device_id_type=MESH)

    def greet_line(i):
        pl.semaphore_signal(barrier, inc=1, device_id=line((me + i) % 8), device_id_type=MESH)

    loop(16, greet_plane, 1)
    loop(8, greet_line, 1)

    loads[0].wait()
    image_unit, image_len = unit_rows(image[...])
    cols[0] = image_unit.astype(BF16)

    def text_block(r):
        unit, _ = unit_rows(text[rows(r * 128), :])
        low = unit.astype(BF16)
        tlow[rows(r * 128), :] = low
        tlow_t[:, rows(r * 128)] = low.astype(F32).T.astype(BF16)
        row_m[rows(r * 128), :] = jnp.full((128, 128), LOW, F32)
        row_s[rows(r * 128), :] = jnp.zeros((128, 128), F32)

    pl.semaphore_wait(barrier, 22)

    def ag_send(dz, dy, lo, size, ez, ey):
        there = slot(dz - ez, dy - ey)
        copy = copy_to(
            cols.at[slot(dz, dy), lo : lo + size],
            cols.at[there, lo : lo + size],
            cols_ss.at[len(sends)],
            cols_rs.at[there * 4 + lo // 32],
            {"dp": plane(ez, ey)},
        )
        copy.start()
        sends.append(copy)

    def ag_wait(dz, dy, lo, size):
        here = slot(dz, dy)
        block = cols.at[here, lo : lo + size]
        copy_to(block, block, cols_ss.at[0], cols_rs.at[here * 4 + lo // 32], {"dp": dp}).wait_recv()

    def flip(swap, *pair):
        return pair[::-1] if swap else pair

    def half_send(swap, first, second, to_first, to_second, lo=0, size=64):
        dz, dy = flip(swap, first, second)
        ez, ey = flip(swap, to_first, to_second)
        ag_send(dz, dy, lo + 64 * swap, size, ez, ey)

    def half_wait(swap, first, second, lo=0, size=64):
        dz, dy = flip(swap, first, second)
        ag_wait(dz, dy, lo + 64 * swap, size)

    for to in ((0, 1), (0, 3), (1, 0), (3, 0), (0, 2)):
        for swap in (0, 1):
            half_send(swap, 0, 0, *to)

    right, left, opposite = (x + 1) % 4, (x + 3) % 4, (x + 2) % 4
    weights = (wi_all, wo_all)

    def weight_rows(turn, lo=0, size=256):
        return pl.ds(pl.multiple_of((y + z + turn) % 2 * 256 + lo, 64), size)

    def wx(n, which, src, dst, chip):
        at = weight_rows(0)
        ref = weights[which]
        return copy_to(
            ref.at[src, core, at], ref.at[dst, core, at], wx_ss.at[n], wx_rs.at[which * 4 + dst], line(chip * 2 + core)
        )

    wx_plan = ((0, 0, 2, right), (1, 0, 1, left), (1, 0, 2, right), (0, 0, 1, left), (0, 2, 3, right), (1, 1, 3, left))

    def wx_wait(which, rel):
        block = weights[which].at[rel, core, weight_rows(0)]
        copy_to(block, block, wx_ss.at[0], wx_rs.at[which * 4 + rel], line(me)).wait_recv()

    def wy_block(part, j, turn):
        which, first, count = ((0, 1, 2), (0, 3, 1), (1, 1, 3))[part]
        return weights[which].at[pl.ds(first, count), core, weight_rows(turn, j * 64, 64)]

    def wy(part, j):
        dz, dy = AROUND[j]
        block = wy_block(part, j, 0)
        n = part * 4 + j
        return copy_to(block, block, wy_ss.at[n], wy_rs.at[n], {"dp": plane(4 - dz, 4 - dy)})

    def wy_wait(part, j):
        block = wy_block(part, j, 1)
        n = part * 4 + j
        copy_to(block, block, wy_ss.at[n], wy_rs.at[n], {"dp": dp}).wait_recv()

    def wd(which, j, side):
        if j < 0:
            block = weights[which].at[0, side]
        else:
            at = weight_rows(0) if j == 4 else weight_rows(1, j * 64, 64)
            block = weights[which].at[pl.ds(1, 3), side, at]
        n = which * 6 + j + 1
        return copy_to(block, block, wd_ss.at[n], wd_rs.at[n], line(x * 2 + 1 - core))

    twin = (1 - section) * 4 + mp
    h_copy = copy_to(hin.at[rows(twin * 128), :], hother, h_s.at[0], h_s.at[1], line(twin))
    for load in loads[2:]:
        load.wait()
    for n in range(4):
        wx(n, *wx_plan[n]).start()
    for which in (0, 1):
        wd(which, -1, core).start()
    h_copy.start()

    def score_pair(p):
        pair = cols[pl.ds(2 * p, 2)].reshape(256, 512)
        part = dot_nt(tlow[...], pair)
        c_m, c_s = jnp.full((8, 256), LOW, F32), jnp.zeros((8, 256), F32)
        for r in range(8):
            at = slice(r * 128, (r + 1) * 128)
            s = part[at] * mult2
            scores[p, at, :] = s
            s3 = s.reshape(16, 8, 256)
            n_m = jnp.maximum(c_m, jnp.max(s3, axis=0))
            c_s = c_s * jnp.exp2(c_m - n_m) + jnp.sum(jnp.exp2(s3 - n_m[None]), axis=0)
            c_m = n_m
            old = row_m[at, :]
            s0, s1 = s[:, :128], s[:, 128:]
            new = jnp.maximum(old, jnp.maximum(s0, s1))
            row_s[at, :] = row_s[at, :] * jnp.exp2(old - new) + jnp.exp2(s0 - new) + jnp.exp2(s1 - new)
            row_m[at, :] = new

        peak = jnp.max(c_m, axis=0, keepdims=True)
        total = peak + jnp.log2(jnp.sum(c_s * jnp.exp2(c_m - peak), axis=0, keepdims=True))
        for j in (0, 1):
            own_stat[pl.ds(2 * p + j, 1), :] = total[:, j * 128 : (j + 1) * 128]

    def spread(swap, first, second):
        for to in (1, 3):
            half_send(swap, first, second, to, 0)

    both = (0, 1)
    loads[1].wait()
    loop(8, text_block)
    for swap in both:
        half_wait(swap, 0, 1)
        half_wait(swap, 0, 3)
    for swap in both:
        spread(swap, 0, 1)
        spread(swap, 0, 3)
    for swap in both:
        half_wait(swap, 1, 0)
        half_send(swap, 1, 0, 3, 0)
        half_wait(swap, 3, 0)
    loop(2, score_pair)
    for swap in both:
        half_wait(swap, 0, 2)
        spread(swap, 0, 2)
    for swap in both:
        for second in (1, 3):
            half_wait(swap, 3, second)
            half_send(swap, 3, second, 1, 0)
            half_wait(swap, 1, second)
    wx_wait(0, 2)
    wx(4, *wx_plan[4]).start()
    wx_wait(1, 1)
    wx(5, *wx_plan[5]).start()
    loop(4, score_pair, 2)
    for swap in both:
        half_wait(swap, 2, 0)
    loop(5, score_pair, 4)
    for swap in both:
        half_wait(swap, 1, 2)
        half_send(swap, 1, 2, 3, 0)
        half_wait(swap, 3, 2)
    half_wait(1, 2, 1)
    loop(6, score_pair, 5)
    half_wait(0, 2, 1)
    for swap in both:
        half_wait(swap, 2, 3)
    wx_wait(0, 1)
    for j in range(4):
        wy(0, j).start()
    loop(7, score_pair, 6)
    for swap in both:
        half_wait(swap, 2, 2)
    score_pair(7)
    for k, (dz, dy) in enumerate(ORDER):
        cst[pl.ds(plane(dz, dy), 1), :] = own_stat[k : k + 1, :]

    def cst_copy(k):
        dz, dy = ORDER[k]
        return copy_to(cst, cst_in.at[dp], cst_ss.at[k], cst_rs.at[dp], {"dp": plane(dz, dy)})

    def cst_wait(k):
        copy_to(cst, cst_in.at[away(k)], cst_ss.at[k], cst_rs.at[away(k)], {"dp": dp}).wait_recv()

    for k in range(15, 0, -1):
        cst_copy(k).start()
    cst_in[dp] = cst[...]

    for r in range(8):
        m_t = row_m[r * 128 : (r + 1) * 128, :].T
        s_t = row_s[r * 128 : (r + 1) * 128, :].T
        peak = jnp.max(m_t, axis=0, keepdims=True)
        rst[r : r + 1, :] = peak + jnp.log2(jnp.sum(s_t * jnp.exp2(m_t - peak), axis=0, keepdims=True))

    def rst_copy(i):
        q = (me + i) % 8
        return copy_to(rst, rst_in.at[me], rst_ss.at[i], rst_rs.at[me], line(q))

    def rst_wait(i):
        q = (me + i) % 8
        copy_to(rst, rst_in.at[q], rst_ss.at[i], rst_rs.at[q], line(me)).wait_recv()

    loop(8, lambda i: rst_copy(i).start(), 1)
    rst_in[me] = rst[...]

    def hidden_block(r):
        at = rows(r * 128)
        h = hin[at, :]
        pre = dot_nn(h, wi_all[0, core])
        sig = jax.nn.sigmoid(1.702 * pre)
        act[at, :] = (pre * sig).astype(BF16)
        slope[at, :] = sig + 1.702 * pre * sig * (1.0 - sig)
        hin_t[:, at] = h.astype(F32).T.astype(BF16)

    loop(8, hidden_block)

    loop(8, rst_wait, 1)
    peak = jnp.max(rst_in[...], axis=0)
    total = jnp.sum(jnp.exp2(rst_in[...] - peak[None]), axis=0)
    rst_a[...] = peak + jnp.log2(2.0 * total)
    for r in range(8):
        row_a[r * 128 : (r + 1) * 128, :] = jnp.broadcast_to(rst_a[r : r + 1, :], (128, 128)).T

    loop(16, cst_wait, 1)
    peak = jnp.max(cst_in[...], axis=0)
    total = jnp.sum(jnp.exp2(cst_in[...] - peak[None]), axis=0)
    own_stat[...] = peak + jnp.log2(2.0 * total)
    for k, (dz, dy) in enumerate(ORDER):
        col_b[k : k + 1, :] = own_stat[pl.ds(plane(dz, dy), 1), :]

    def pass_copy(chip):
        other = chip * 2 + 1 - core
        return copy_to(tshare.at[other], tpass.at[chip], tp_ss.at[chip], tp_rs.at[chip], line(x * 2 + 1 - core))

    def tshare_copy(chip):
        own = chip * 2 + core
        return copy_to(tshare.at[own], tshare_in.at[x], ts_ss.at[chip], ts_rs.at[x], line(own))

    chips = (opposite, right, left, x)
    parts = (grads0, grads1, grads2, grads3)
    mine = 2 * mp + section
    eye = (
        lax.broadcasted_iota(jnp.int32, (128, 128), 0) == lax.broadcasted_iota(jnp.int32, (128, 128), 1)
    ).astype(F32)

    def make_grads(i):
        for half in both:
            at = rows(chips[i] * 256 + half * 128)
            a = row_a[at, :]
            for k in range(16):
                p, j = k // 2, k % 2
                s = scores[p, at, j * 128 : (j + 1) * 128]
                part = jnp.exp2(s - a) + jnp.exp2(s - col_b[k : k + 1, :])
                if k == 0:
                    part = part - eye * jnp.where(chips[i] * 2 + half == mine, 1.0, 0.0)
                parts[i][half * 128 : (half + 1) * 128, k * 128 : (k + 1) * 128] = part.astype(BF16)

    def text_merge(chip):
        own = chip * 2 + core
        pass_copy(chip).wait_recv()
        tshare[own] = (tshare[own].astype(F32) + tpass[chip].astype(F32)).astype(BF16)

    def wd_pass(which):
        for j in range(4):
            for part in ((0, 1), (2,))[which]:
                wy_wait(part, j)
            wd(which, j, core).start()

    def wd_wait(which):
        for j in range(-1, 5):
            wd(which, j, 1 - core).wait_recv()

    wx_wait(1, 2)
    for which in both:
        wx_wait(which, 3)
    for part in (1, 2):
        for j in range(4):
            wy(part, j).start()
    for which in both:
        wd(which, 4, core).start()
    make_grads(0)
    for i in range(4):
        if i < 3:
            make_grads(i + 1)
        part = dot_nn(parts[i][...], cols[...].reshape(2048, 512))
        for j in (0, 1):
            tshare[chips[i] * 2 + j] = part[j * 128 : (j + 1) * 128].astype(BF16)
        pass_copy(chips[i]).start()
        if i > 0:
            text_merge(chips[i - 1])
            tshare_copy(chips[i - 1]).start()
    text_merge(x)
    wd_pass(0)

    def image_part(p):
        part = sum(
            dot_nn(tlow_t[:, rows(chips[i] * 256, 256)], parts[i][:, p * 256 : (p + 1) * 256]) for i in range(4)
        )
        for j in (0, 1):
            dz, dy = ORDER[2 * p + j]
            block = part[:, j * 128 : (j + 1) * 128].astype(BF16)
            ishare[0, dz, dy] = block[:256]
            ishare[1, dy, dz] = block[256:]

    def step_of(swap, far):
        return {"dp": plane(*flip(swap, far, 0))}

    def image_far(n, swap):
        src, dst, to = (
            (ishare.at[swap, 2, 0:2], relay_in.at[swap, 0], 1),
            (ishare.at[swap, 2, 2:4], relay_in.at[swap, 1], 3),
            (ishare.at[swap, 1, 2:4], ifar_in.at[swap, 0, 2:4], 1),
            (ishare.at[swap, 3, 0:2], ifar_in.at[swap, 1, 0:2], 3),
            (joined.at[swap, 0], ifar_in.at[swap, 0, 0:2], 1),
            (joined.at[swap, 1], ifar_in.at[swap, 1, 2:4], 3),
        )[n]
        k = swap * 6 + n
        return copy_to(src, dst, if_ss.at[k], if_rs.at[k], step_of(swap, to))

    def image_near(swap, far):
        n = swap * 3 + 3 - far
        return copy_to(isum.at[swap, far], inear_in.at[swap, 3 - far], ir_ss.at[n], ir_rs.at[n], step_of(1 - swap, far))

    for p in range(7, -1, -1):
        image_part(p)
    for n in range(4):
        for swap in both:
            image_far(n, swap).start()

    def image_relay():
        for n, far, lo in ((0, 1, 0), (1, 3, 2)):
            for swap in both:
                image_far(n, swap).wait_recv()
                joined[swap, n] = (
                    ishare[swap, far, lo : lo + 2].astype(F32) + relay_in[swap, n].astype(F32)
                ).astype(BF16)
                image_far(n + 4, swap).start()


    wd_pass(1)
    h_copy.wait_recv()

    wd_wait(0)

    def home(q):
        turn = (q // 2 + 4 - x) % 4
        return jnp.where(turn == 2, 3, jnp.where(turn == 3, 2, turn)), q % 2

    def own_block(r):
        h = jnp.where(r // 4 == section, hin[rows(me * 128), :], hother[...])
        slope_own[r] = slope_of(dot_nn(h, wi_all[home(r)]))

    loop(8, own_block, 4)

    def tshare_sum(i, acc):
        chip = (x + i) % 4
        copy_to(tshare.at[0], tshare_in.at[chip], ts_ss.at[chip], ts_rs.at[chip], line(me)).wait_recv()
        return acc + tshare_in[chip].astype(F32)

    total = lax.fori_loop(1, 4, tshare_sum, tshare[me].astype(F32)) * mult
    unit, length = unit_rows(text[rows(me * 128), :])
    gown[0] = unit_backward(unit, length, total).astype(BF16)

    sibling = x + 1 - 2 * (x % 2)

    def g_copy(layer, half, sems):
        at = pl.ds(half * 64, 64)
        to = jnp.where(section == layer, sibling, 3 - x) * 2 + core
        return copy_to(gown.at[1 - layer, at], gbuf.at[me, at], sems.at[half], g_rs.at[me * 2 + half], line(to))

    def g_send(layer, sems):
        for half in both:
            g_copy(layer, half, sems).start()

        @pl.when(section == layer)
        def _():
            gbuf[me] = gown[1 - layer]

    def g_forward(half):
        q = (3 - x) * 2 + core
        block = gbuf.at[q, pl.ds(half * 64, 64)]
        return copy_to(block, block, gf_ss.at[half], g_rs.at[q * 2 + half], line(sibling * 2 + core))

    def g_arrive(chip):
        q = chip * 2 + core
        for half in both:
            block = gbuf.at[q, pl.ds(half * 64, 64)]
            copy_to(block, block, gf_ss.at[0], g_rs.at[q * 2 + half], line(me)).wait_recv()

    def order_of(i):
        return jnp.where(i == 0, x, jnp.where(i == 1, sibling, jnp.where(i == 2, 3 - x, 3 - sibling)))

    def g_pass(i):
        chip = order_of(i)
        block = gbuf.at[chip * 2 + core]
        return copy_to(block, block, gp_ss.at[i], gp_rs.at[chip], line(x * 2 + 1 - core))

    def g_passed(chip):
        block = gbuf.at[chip * 2 + 1 - core]
        copy_to(block, block, gp_ss.at[0], gp_rs.at[chip], line(me)).wait_recv()

    def chain(layer):
        g = gown[1 - layer]

        def step(j, acc):
            q = layer * 4 + j
            back = dot_nt(g, wo_all[home(q)])
            pre_grad = (back * slope_own[q]).astype(BF16)
            return acc + dot_nt(pre_grad, wi_all[home(q)])

        return lax.fori_loop(0, 4, step, g.astype(F32)).astype(BF16)

    wd_wait(1)
    g_send(1, g1_ss)
    gown[1] = chain(1)
    g_send(0, g0_ss)
    loop(4, own_block)
    image_relay()
    lowest = chain(0)
    gin[0] = lowest[:, :256]
    gin[1] = lowest[:, 256:]

    def in_copy(i):
        q = (me + i) % 8
        return copy_to(gin.at[q // 4], inbuf.at[me], in_ss.at[i], in_rs.at[me], line(q))

    def image_fold(swap):
        for n in range(2, 6):
            image_far(n, swap).wait_recv()
        total = ishare[swap, 0].astype(F32) + ifar_in[swap, 0].astype(F32) + ifar_in[swap, 1].astype(F32)
        isum[swap] = total.astype(BF16)
        for far in (2, 1, 3):
            image_near(swap, far).start()

    def weight_rows_of(i):
        chip = order_of(i)
        g_passed(chip)
        at = rows(chip * 256, 256)
        g = gbuf[pl.ds(2 * chip, 2)].reshape(256, 512)
        out_part = dot_tn(g, act[at, :])
        pre_grad = (dot_nt(g, wo_all[0, core]) * slope[at, :]).astype(BF16)
        in_part = dot_nn(hin_t[:, at], pre_grad)

        @pl.when(i == 0)
        def _():
            wacc[1] = out_part
            wacc[0] = in_part

        @pl.when(i > 0)
        def _():
            wacc[1] += out_part
            wacc[0] += in_part

    def weight_step(i):
        @pl.when(i < 4)
        def _():
            pl.when(i % 2 == 1)(lambda: g_arrive(order_of(i)))
            pl.when(i != 2)(lambda: g_pass(i).start())

        @pl.when(i == 4)
        def _():
            loop(8, lambda k: in_copy(k).start(), 1)
            inbuf[me] = gin[section]

        @pl.when(i == 2)
        def _():
            for swap in both:
                image_fold(swap)

        pl.when(i > 0)(lambda: weight_rows_of(i - 1))

    for half in both:
        q = (3 - x) * 2 + core
        block = gbuf.at[q, pl.ds(half * 64, 64)]
        copy_to(block, block, gf_ss.at[0], g_rs.at[q * 2 + half], line(me)).wait_recv()
        g_forward(half).start()
    g_pass(2).start()
    loop(5, weight_step)

    def put_weight(which, value):
        for zz in range(4):
            for yy in range(4):
                block = value[(zz * 4 + yy) * 32 : (zz * 4 + yy + 1) * 32].astype(BF16)
                wg[which, 0, zz, yy] = block[:, :256]
                wg[which, 1, yy, zz] = block[:, 256:]

    def weight_far(which, swap, n):
        first = y if swap else z
        block = wg.at[which, swap]
        landed = wfar_in.at[which, swap]
        src, dst, to = (
            (block.at[(first + 2) % 4, 0:2], wrelay_in.at[which, swap, 0], 1),
            (block.at[(first + 2) % 4, 2:4], wrelay_in.at[which, swap, 1], 3),
            (block.at[(first + 1) % 4, 2:4], landed.at[0, 2:4], 1),
            (block.at[(first + 3) % 4, 0:2], landed.at[1, 0:2], 3),
            (wjoined.at[which, swap, 0], landed.at[0, 0:2], 1),
            (wjoined.at[which, swap, 1], landed.at[1, 2:4], 3),
        )[n]
        k = which * 12 + swap * 6 + n
        return copy_to(src, dst, wf_ss.at[k], wf_rs.at[k], step_of(swap, to))

    def weight_relay(which):
        for n, far, lo in ((0, 1, 0), (1, 3, 2)):
            for swap in both:
                weight_far(which, swap, n).wait_recv()
                block = wg[which, swap, ((y if swap else z) + far) % 4, lo : lo + 2]
                wjoined[which, swap, n] = (
                    block.astype(F32) + wrelay_in[which, swap, n].astype(F32)
                ).astype(BF16)
                weight_far(which, swap, n + 4).start()

    def weight_near(which, swap, far):
        n = which * 6 + swap * 3 + 3 - far
        at = ((z if swap else y) + far) % 4
        return copy_to(
            wsum.at[which, swap, at], wnear_in.at[which, swap, 3 - far], wn_ss.at[n], wn_rs.at[n], step_of(1 - swap, far)
        )

    def weight_start(which, messages):
        for n in messages:
            for swap in both:
                weight_far(which, swap, n).start()

    def weight_fold(which):
        for swap in both:
            for n in range(2, 6):
                weight_far(which, swap, n).wait_recv()
            total = wg[which, swap, y if swap else z].astype(F32)
            for side in both:
                total = total + wfar_in[which, swap, side].astype(F32)
            wsum[which, swap] = total.astype(BF16)
        for far in (2, 1, 3):
            for swap in both:
                weight_near(which, swap, far).start()

    def weight_end(which, out):
        for swap in both:
            total = wsum[which, swap, z if swap else y].astype(F32)
            for far in (1, 2, 3):
                landed = wnear_in.at[which, swap, far - 1]
                n = which * 6 + swap * 3 + far - 1
                copy_to(landed, landed, wn_ss.at[n], wn_rs.at[n], {"dp": dp}).wait_recv()
                total = total + landed[...].astype(F32)
            out[0, :, swap * 256 : (swap + 1) * 256] = total

    put_weight(1, wacc[1])
    weight_start(1, (0, 1))
    put_weight(0, wacc[0])
    weight_start(0, (0, 1))
    weight_start(1, (2, 3))
    weight_start(0, (2, 3))

    for copy in sends:
        copy.wait_send()
    h_copy.wait_send()
    for n in range(6):
        wx(n, *wx_plan[n]).wait_send()
    for which in both:
        for j in range(-1, 5):
            wd(which, j, core).wait_send()
    for part in range(3):
        for j in range(4):
            wy(part, j).wait_send()
    for k in range(1, 16):
        cst_copy(k).wait_send()
    loop(8, lambda i: rst_copy(i).wait_send(), 1)
    loop(4, lambda i: pass_copy(i).wait_send())
    loop(4, lambda i: tshare_copy((x + i) % 4).wait_send(), 1)
    weight_relay(1)
    weight_relay(0)
    for swap in both:
        total = isum[swap, 0].astype(F32)
        for far in (1, 2, 3):
            landed = inear_in.at[swap, far - 1]
            copy_to(landed, landed, ir_ss.at[0], ir_rs.at[swap * 3 + far - 1], {"dp": dp}).wait_recv()
            total = total + landed[...].astype(F32)
        ifull[:, swap * 256 : (swap + 1) * 256] = total.T
    total = ifull[...] * mult
    image_unit, image_len = unit_rows(image[...])
    ihalf[0] = unit_backward(image_unit, image_len, total).astype(BF16)
    ihalf_copy = copy_to(ihalf.at[0], ihalf.at[1], ih_s.at[0], ih_s.at[1], line(twin))
    ihalf_copy.start()
    weight_fold(1)

    def in_wait(i):
        q = (me + i) % 8
        copy_to(gin.at[0], inbuf.at[q], in_ss.at[i], in_rs.at[q], line(me)).wait_recv()

    loop(8, in_wait, 1)
    input_out[...] = inbuf[...].reshape(1024, 256)

    weight_fold(0)
    image_out[rows(section * 128), :] = ihalf[0]
    ihalf_copy.wait_recv()
    image_out[rows((1 - section) * 128), :] = ihalf[1]
    weight_end(1, second_out)
    weight_end(0, first_out)
    for swap in both:
        for far in (1, 2, 3):
            image_near(swap, far).wait_send()
        for n in range(6):
            image_far(n, swap).wait_send()
    ihalf_copy.wait_send()
    for layer, sems in ((1, g1_ss), (0, g0_ss)):
        for half in both:
            g_copy(layer, half, sems).wait_send()
    for half in both:
        g_forward(half).wait_send()
    loop(4, lambda i: g_pass(i).wait_send())
    loop(8, lambda i: in_copy(i).wait_send(), 1)
    for which in both:
        for swap in both:
            for far in (1, 2, 3):
                weight_near(which, swap, far).wait_send()
            for n in range(6):
                weight_far(which, swap, n).wait_send()


def settle(*refs):
    sems = refs[8]
    copies = [pltpu.make_async_copy(src, dst, sems.at[n]) for n, (src, dst) in enumerate(zip(refs[:4], refs[4:8]))]
    for copy in copies:
        copy.start()
    for copy in copies:
        copy.wait()


def body(text_feats, image_feats, logit_scale, layer_inputs, w_in, w_out):
    vmem = pl.BlockSpec(memory_space=pltpu.VMEM)
    dma = pltpu.SemaphoreType.DMA
    scratch = [
        pltpu.VMEM((1024, 512), BF16),
        pltpu.VMEM((128, 512), BF16),
        pltpu.VMEM((1024, 512), BF16),
        pltpu.VMEM((16, 128, 512), BF16),
        pltpu.VMEM((1024, 512), BF16),
        pltpu.VMEM((512, 1024), BF16),
        pltpu.VMEM((8, 1024, 256), F32),
        *[pltpu.VMEM((256, 2048), BF16)] * 4,
        pltpu.VMEM((1024, 128), F32),
        pltpu.VMEM((1024, 128), F32),
        pltpu.VMEM((1024, 128), F32),
        pltpu.VMEM((8, 128), F32),
        pltpu.VMEM((8, 8, 128), F32),
        pltpu.VMEM((8, 128), F32),
        pltpu.VMEM((16, 128), F32),
        pltpu.VMEM((16, 128), F32),
        pltpu.VMEM((16, 16, 128), F32),
        pltpu.VMEM((16, 128), F32),
        pltpu.VMEM((8, 128, 512), BF16),
        pltpu.VMEM((4, 128, 512), BF16),
        pltpu.VMEM((4, 128, 512), BF16),
        pltpu.VMEM((2, 4, 4, 256, 128), BF16),
        pltpu.VMEM((2, 2, 2, 256, 128), BF16),
        pltpu.VMEM((2, 2, 2, 256, 128), BF16),
        pltpu.VMEM((2, 2, 4, 256, 128), BF16),
        pltpu.VMEM((2, 4, 256, 128), BF16),
        pltpu.VMEM((2, 3, 256, 128), BF16),
        pltpu.VMEM((128, 512), F32),
        pltpu.VMEM((2, 128, 512), BF16),
        pltpu.VMEM((4, 2, 512, 512), BF16),
        pltpu.VMEM((4, 2, 512, 512), BF16),
        pltpu.VMEM((128, 512), BF16),
        pltpu.VMEM((1024, 512), BF16),
        pltpu.VMEM((1024, 512), F32),
        pltpu.VMEM((8, 128, 512), F32),
        pltpu.VMEM((512, 1024), BF16),
        pltpu.VMEM((8, 128, 512), BF16),
        pltpu.VMEM((2, 128, 256), BF16),
        pltpu.VMEM((2, 128, 512), BF16),
        pltpu.VMEM((8, 128, 256), BF16),
        pltpu.VMEM((2, 512, 512), F32),
        pltpu.VMEM((2, 2, 4, 4, 32, 256), BF16),
        pltpu.VMEM((2, 2, 2, 2, 32, 256), BF16),
        pltpu.VMEM((2, 2, 2, 2, 32, 256), BF16),
        pltpu.VMEM((2, 2, 2, 4, 32, 256), BF16),
        pltpu.VMEM((2, 2, 4, 32, 256), BF16),
        pltpu.VMEM((2, 2, 3, 32, 256), BF16),
        dma((5,)),
        dma((32,)), dma((64,)),
        dma((6,)), dma((8,)), dma((12,)), dma((12,)), dma((12,)), dma((12,)),
        dma((2,)),
        dma((8,)), dma((8,)),
        dma((16,)), dma((16,)),
        dma((4,)), dma((4,)), dma((4,)), dma((4,)),
        dma((12,)), dma((12,)), dma((6,)), dma((6,)),
        dma((2,)),
        dma((2,)), dma((2,)), dma((2,)), dma((16,)), dma((4,)), dma((4,)),
        dma((8,)), dma((8,)),
        dma((24,)), dma((24,)), dma((12,)), dma((12,)),
    ]
    results = pl.pallas_call(
        kernel,
        out_shape=(
            pltpu.VMEM((256, 512), BF16),
            pltpu.VMEM((1024, 256), BF16),
            pltpu.VMEM((1, 32, 512), F32),
            pltpu.VMEM((1, 32, 512), F32),
        ),
        in_specs=[pl.BlockSpec(memory_space=pltpu.SMEM)] + [pl.BlockSpec(memory_space=pl.ANY)] * 5,
        out_specs=(vmem,) * 4,
        scratch_shapes=scratch,
        compiler_params=pltpu.CompilerParams(
            collective_id=0, has_side_effects=True, vmem_limit_bytes=54 * 1024 * 1024
        ),
    )(logit_scale, text_feats, image_feats, layer_inputs, w_in, w_out)
    results = [pltpu.with_memory_space_constraint(r, pltpu.VMEM) for r in results]
    return pl.pallas_call(
        settle,
        out_shape=tuple(jax.ShapeDtypeStruct(r.shape, r.dtype) for r in results),
        in_specs=[vmem] * 4,
        out_specs=(pl.BlockSpec(memory_space=pl.ANY),) * 4,
        scratch_shapes=[dma((4,))],
    )(*results)


def solution(mesh):
    placed = (
        P("dp", None),
        P(("dp", "mp"), None),
        P(),
        P("section", "dp", None),
        P("section", None, "mp"),
        P("section", "mp", None),
    )
    return jax.shard_map(
        body,
        mesh=mesh,
        in_specs=placed,
        out_specs=(
            P(("dp", "mp"), None),
            P("dp", "section"),
            P("section", "dp", "mp"),
            P("section", "dp", "mp"),
        ),
        check_vma=False,
    )
```
